128 devices in a mesh: rows: 16 (over y, z), groups: 8 (over x, core).
Axes of the slice: x: 4, y: 4, z: 4, core: 2. Of those that a mesh axis runs over, the one named last changes fastest.
Arguments:
- basis: bfloat16 [8, 524288, 128], P(None, ('rows', 'groups')), may hold values from -6 to 6
- image: bfloat16 [8, 524288, 128], P(None, ('rows', 'groups')), may hold values from -6 to 6
- selection: int32 [8, 64], replicated, may hold values from 0 to 127, all different within a row
Outputs:
- rotated: bfloat16 [8, 524288, 128], P(None, ('rows', 'groups'))
The draws below stay inside these ranges and needn't reach their ends.
Inputs may be any that keep to these rules, and one draw needn't show every extreme that they name: Each row of selection names 64 different columns.
All inputs are finite; a program needn't handle non-finite values.
Results may differ from the reference program's by a relative error of at most 0.005.
Values may be sent and summed in bfloat16 or wider, within the bound.
A program may use at most 128 MiB of HBM per device.

```python
import jax
import jax.numpy as jnp
from jax import lax

RECYCLE = 64
COLS = 128
NSYS = 8
ITERS = 3
NROWS = 524288


def levels(own_key, shape, shards, smallest, largest):
    gain = 1.0
    for position, shards_of in shards:
        steps = jax.random.uniform(jax.random.fold_in(jax.random.fold_in(own_key, 6), position), (shards_of,), jnp.float32, smallest / len(shards), largest / len(shards))
        gain = gain * jnp.repeat(jnp.exp(steps), shape[position] // shards_of).reshape((-1,) + (1,) * (len(shape) - 1 - position))
    return gain


def picks_of(rng, rows, amount, top, lift):
    sequence = jax.random.permutation(jax.random.fold_in(rng, 1), amount)
    favour = sequence
    for power in range(3):
        favour = favour * favour // amount
    favour = favour * lift // amount
    chance = jax.random.randint(jax.random.fold_in(rng, 2), (rows, amount), 0, 4096) + favour
    sure = jax.random.permutation(jax.random.fold_in(rng, 3), rows)[jnp.arange(amount) % rows]
    chance = jnp.where(jnp.arange(rows)[:, None] == sure[None, :], 1 << 14, chance)
    merit = chance * amount + jnp.arange(amount)
    return lax.top_k(merit.astype(jnp.int32), top)[1].astype(jnp.int32)


def noise(key, dims, scale, limit, split=(), kind=jnp.bfloat16):
    gain = levels(key, dims, split, -0.22, 0.18) if split else 1.0
    values = jax.random.normal(key, dims, jnp.float32) * scale * gain
    return jnp.minimum(jnp.maximum(values, -limit), limit).astype(kind)


def setup_inputs(seed: int = 0) -> dict:
    streams_of = jax.random.split(jax.random.key(seed), 4)
    basis = noise(streams_of[0], (NSYS, NROWS, COLS), 1.0, 6.0, ((1, 128),))
    image = noise(streams_of[1], (NSYS, NROWS, COLS), 1.0, 6.0, ((1, 128),))
    selection = picks_of(streams_of[2], NSYS, COLS, RECYCLE, 0)
    return dict(basis=basis, image=image, selection=selection)


def small_solve(grams, chosen):
    gram_s, cross, gram_f = (grams[0], grams[1], grams[2])
    width = gram_s.shape[0]
    coeffs = (jnp.arange(width, dtype=jnp.int32)[:, None] == chosen[None, :]).astype(jnp.float32)
    factor = jnp.linalg.cholesky(gram_f)
    for step in range(ITERS):
        moved = jnp.dot(cross.T, coeffs, precision=lax.Precision.HIGHEST)
        halfway = lax.linalg.triangular_solve(factor, moved, left_side=True, lower=True)
        solved = lax.linalg.triangular_solve(factor, halfway, left_side=True, lower=True, transpose_a=True)
        metric = jnp.dot(solved.T, jnp.dot(gram_s, solved, precision=lax.Precision.HIGHEST), precision=lax.Precision.HIGHEST) / NROWS
        lower = jnp.linalg.cholesky(metric)
        coeffs = lax.linalg.triangular_solve(lower, solved, left_side=False, lower=True, transpose_a=True)
    return coeffs

def one_system(items):
    left, right, chosen = items
    gram_s = jnp.dot(left.T.astype(jnp.float32), left.astype(jnp.float32), preferred_element_type=jnp.float32)
    cross = jnp.dot(left.T.astype(jnp.float32), right.astype(jnp.float32), preferred_element_type=jnp.float32)
    gram_f = jnp.dot(right.T.astype(jnp.float32), right.astype(jnp.float32), preferred_element_type=jnp.float32)
    coeffs = small_solve(jnp.stack([gram_s, cross, gram_f]), chosen).astype(jnp.bfloat16)
    first = jnp.dot(left.astype(jnp.float32), coeffs.astype(jnp.float32), preferred_element_type=jnp.float32)
    second = jnp.dot(right.astype(jnp.float32), coeffs.astype(jnp.float32), preferred_element_type=jnp.float32)
    return jnp.concatenate([first, second], axis=1).astype(jnp.bfloat16)

def reference(basis, image, selection):
    return lax.map(one_system, (basis, image, selection))
```

```python
import functools

import jax
import jax.numpy as jnp
from jax import lax
from jax.experimental import pallas as pl
from jax.experimental.pallas import tpu as pltpu
from jax.sharding import PartitionSpec as P

ITERS = 3
F32 = jnp.float32
BF16 = jnp.bfloat16
HIGHEST = lax.Precision.HIGHEST
SYSTEMS = 8
DEPTH = 4096
COLS = 128
KEPT = 64
CHIPS = 64
PLANE = 16


def dot(a, b, over_a, over_b):
    dims = (((over_a,), (over_b,)), ((), ()))
    return lax.dot_general(a, b, dims, precision=HIGHEST, preferred_element_type=F32)


def lane(tile, j):
    return jnp.broadcast_to(tile[:, j : j + 1], (8, 128))


def row(tile, j):
    return jnp.broadcast_to(tile[j : j + 1, :], (8, 128))


def added(parts):
    while len(parts) > 1:
        parts = [parts[i] + parts[i + 1] for i in range(0, len(parts), 2)]
    return parts[0]


def times(cols, tile):
    return added([cols[j] * row(tile, j) for j in range(8)])


def less(tile, cols, rows):
    return tile - added([cols[j] * rows[j] for j in range(8)])


def pivot(v, j, at, r):
    piv = v[j]
    for other in range(8):
        if other != j:
            w = row(v[other], j) * r
            v[other] = jnp.where(at, w, v[other] - piv * w)
    v[j] = jnp.where(at, r, -(piv * r))


def solved_rows(f, x, sub):
    n = len(f)
    for k in range(n):
        cols = [[lane(f[i], 8 * k + j) for j in range(8)] for i in range(n)]
        v = list(cols[k])
        for j in range(8):
            pivot(v, j, sub == j, 1.0 / row(v[j], j))
        fk, xk = times(v, f[k]), times(v, x[k])
        fr = [row(fk, j) for j in range(8)]
        xr = [row(xk, j) for j in range(8)]
        for i in list(range(k + 1, n)) + list(range(k)):
            if k < n - 1:
                f[i] = less(f[i], cols[i], fr)
            x[i] = less(x[i], cols[i], xr)
        f[k], x[k] = fk, xk
    return x


def normalised_rows(m, y, sub):
    n = len(m)
    out = []
    for k in range(n):
        cols = [[lane(m[i], 8 * k + j) for j in range(8)] for i in range(k, n)]
        v = list(cols[0])
        mine = y[k]
        scale = jnp.zeros((8, 128), F32)
        for j in range(8):
            p = row(v[j], j)
            r = 1.0 / p
            at = sub == j
            scale = jnp.where(at, p, scale)
            mine = mine - jnp.where(sub > j, v[j] * r, 0.0) * row(mine, j)
            pivot(v, j, at, r)
        out.append(mine * lax.rsqrt(scale))
        if k < n - 1:
            mk, yk = times(v, m[k]), times(v, y[k])
            mr = [row(mk, j) for j in range(8)]
            yr = [row(yk, j) for j in range(8)]
            for i in range(k + 1, n):
                m[i] = less(m[i], cols[i - k], mr)
                y[i] = less(y[i], cols[i - k], yr)
    return out


def tiles(a):
    return [a[8 * i : 8 * i + 8] for i in range(a.shape[0] // 8)]


def gather_kernel(
    total_rows, w_hbm, q_hbm, chosen_ref, out_ref,
    wq, lent, given, sums, arrived, pieces, coeffs, local_coeffs,
    load_sem, lent_sem, given_sem, send_sem, recv_sem,
    share_send, share_recv, done_send, done_recv,
):
    me_row, me_group = lax.axis_index("rows"), lax.axis_index("groups")
    x, core = me_group // 2, lax.rem(me_group, 2)
    y, z = me_row // 4, lax.rem(me_row, 4)

    def system(step):
        hop = (2, 1, 3, 0)[step // 2]
        parity = 1 - core if step % 2 == 0 else core
        return 2 * lax.rem(x + hop, 4) + parity

    def load(step):
        s = system(step)
        return [
            pltpu.make_async_copy(ref.at[s], wq.at[step, :, pl.ds(off, COLS)], load_sem.at[step, i])
            for i, (ref, off) in enumerate(((w_hbm, 0), (q_hbm, COLS)))
        ]

    ahead = 4
    for step in range(ahead):
        for copy in load(step):
            copy.start()

    barrier = pltpu.get_barrier_semaphore()

    def at_chip(i):
        dx, dy, dz = i // 16, lax.rem(i // 4, 4), lax.rem(i, 4)
        rows = lax.rem(y + dy, 4) * 4 + lax.rem(z + dz, 4)
        return rows, lax.rem(x + dx, 4)

    def greet(i, _):
        rows, chip_x = at_chip(i)
        pl.semaphore_signal(
            barrier, inc=1, device_id={"rows": rows, "groups": 2 * chip_x + core},
            device_id_type=pl.DeviceIdType.MESH,
        )
        return 0

    lax.fori_loop(1, CHIPS, greet, 0)
    for hop in range(4):
        pl.semaphore_signal(
            barrier, inc=1,
            device_id={"rows": me_row, "groups": 2 * lax.rem(x + hop, 4) + 1 - core},
            device_id_type=pl.DeviceIdType.MESH,
        )

    def gram(step, ref):
        for copy in load(step):
            copy.wait()
        block = wq[step]
        g = lax.dot_general(block, block, (((0,), (0,)), ((), ())), preferred_element_type=F32)
        ref[:, 0:8, :] = g[:COLS, :COLS].reshape(PLANE, 8, COLS)
        ref[:, 8:16, :] = g[COLS:, :COLS].reshape(PLANE, 8, COLS)
        ref[:, 16:24, :] = g[COLS:, COLS:].reshape(PLANE, 8, COLS)
        if step + ahead < 8:
            for copy in load(step + ahead):
                copy.start()

    def lend(k):
        return pltpu.make_async_remote_copy(
            src_ref=lent.at[k], dst_ref=given.at[k], send_sem=lent_sem.at[k], recv_sem=given_sem.at[k],
            device_id={"rows": me_row, "groups": 2 * x + 1 - core}, device_id_type=pl.DeviceIdType.MESH,
        )

    def scatter(k):
        hop = (2, 1, 3, 0)[k]

        def send(j, _):
            rows, chip_x = at_chip(16 * hop + j)
            pltpu.make_async_remote_copy(
                src_ref=sums.at[k, rows], dst_ref=arrived.at[16 * hop + j],
                send_sem=send_sem, recv_sem=recv_sem,
                device_id={"rows": rows, "groups": 2 * chip_x + core}, device_id_type=pl.DeviceIdType.MESH,
            ).start()
            return 0

        if hop == 0:
            arrived[0] = sums[k, me_row]
        lax.fori_loop(1 if hop == 0 else 0, PLANE, send, 0)

    gram(0, lent.at[0])
    pl.semaphore_wait(barrier, CHIPS - 1 + 4)
    lend(0).start()
    for k in range(4):
        gram(2 * k + 1, sums.at[k])
        if k < 3:
            gram(2 * k + 2, lent.at[k + 1])
            lend(k + 1).start()
        lend(k).wait_recv()
        sums[k] = sums[k] + given[k]
        scatter(k)

    others = arrived.at[pl.ds(1, CHIPS - 1)]
    pltpu.make_async_copy(others, others, recv_sem).wait()

    def add(i, total):
        return tuple(t + arrived[i, 8 * n : 8 * n + 8, :] for n, t in enumerate(total))

    total = lax.fori_loop(
        1, CHIPS, add, tuple(arrived[0, 8 * n : 8 * n + 8, :] for n in range(3)), unroll=7
    )
    for n in range(3):
        pieces[me_row, 8 * n : 8 * n + 8, :] = total[n]

    def share(j, _):
        rows, _chip = at_chip(j)
        pltpu.make_async_remote_copy(
            src_ref=pieces.at[me_row], dst_ref=pieces.at[me_row], send_sem=share_send, recv_sem=share_recv,
            device_id={"rows": rows, "groups": me_group}, device_id_type=pl.DeviceIdType.MESH,
        ).start()
        return 0

    lax.fori_loop(1, PLANE, share, 0)
    fifteen = pieces.at[pl.ds(0, PLANE - 1)]
    pltpu.make_async_copy(fifteen, fifteen, share_recv).wait()

    sub = lax.broadcasted_iota(jnp.int32, (8, 128), 0)
    chosen = chosen_ref[pl.ds(me_group, 1), :]
    first = (lax.broadcasted_iota(jnp.int32, (COLS, KEPT), 0) == chosen).astype(F32).T
    gram_s = jnp.concatenate([pieces[i, 0:8, :] for i in range(PLANE)], axis=0)
    step_matrix = jnp.concatenate(
        solved_rows(
            [pieces[i, 16:24, :] for i in range(PLANE)], [pieces[i, 8:16, :] for i in range(PLANE)], sub
        ),
        axis=0,
    )
    metric_step = dot(gram_s, step_matrix, 1, 0)
    coeffs[...] = first

    def iterate(i, _):
        now = coeffs[...]
        moved = dot(now, step_matrix, 1, 1)
        metric = dot(moved, dot(now, metric_step, 1, 1), 1, 1) * (1.0 / total_rows)
        wide = jnp.concatenate([metric, jnp.zeros((KEPT, COLS - KEPT), F32)], axis=1)
        coeffs[...] = jnp.concatenate(normalised_rows(tiles(wide), tiles(moved), sub), axis=0)
        return 0

    lax.fori_loop(0, ITERS, iterate, 0)
    local_coeffs[...] = coeffs[...].astype(BF16)
    out_ref[me_group] = local_coeffs[...]

    def tell(i, _):
        pltpu.make_async_remote_copy(
            src_ref=local_coeffs, dst_ref=out_ref.at[me_group], send_sem=done_send, recv_sem=done_recv,
            device_id={"rows": me_row, "groups": lax.rem(me_group + i, SYSTEMS)},
            device_id_type=pl.DeviceIdType.MESH,
        ).start()
        return 0

    lax.fori_loop(1, SYSTEMS, tell, 0)
    seven = out_ref.at[pl.ds(0, SYSTEMS - 1)]
    pltpu.make_async_copy(seven, seven, done_recv).wait()
    pltpu.make_async_copy(seven, seven, done_send).wait()
    pltpu.make_async_copy(fifteen, fifteen, share_send).wait()
    pltpu.make_async_copy(others, others, send_sem).wait()
    for k in range(4):
        lend(k).wait_send()


def gathered(basis, image, selection, total_rows):
    piece = (24, COLS)
    dma = pltpu.SemaphoreType.DMA
    return pl.pallas_call(
        functools.partial(gather_kernel, total_rows),
        out_shape=jax.ShapeDtypeStruct((SYSTEMS, KEPT, COLS), BF16),
        in_specs=[
            pl.BlockSpec(memory_space=pltpu.HBM),
            pl.BlockSpec(memory_space=pltpu.HBM),
            pl.BlockSpec(memory_space=pltpu.VMEM),
        ],
        out_specs=pl.BlockSpec(memory_space=pltpu.VMEM),
        scratch_shapes=[
            pltpu.VMEM((SYSTEMS, DEPTH, 2 * COLS), BF16),
            pltpu.VMEM((4, PLANE, *piece), F32),
            pltpu.VMEM((4, PLANE, *piece), F32),
            pltpu.VMEM((4, PLANE, *piece), F32),
            pltpu.VMEM((CHIPS, *piece), F32),
            pltpu.VMEM((PLANE, *piece), F32),
            pltpu.VMEM((KEPT, COLS), F32),
            pltpu.VMEM((KEPT, COLS), BF16),
            dma((SYSTEMS, 2)),
            dma((4,)),
            dma((4,)),
            dma, dma, dma, dma, dma, dma,
        ],
        compiler_params=pltpu.CompilerParams(
            collective_id=0, has_side_effects=True, vmem_limit_bytes=40 * 2**20
        ),
        name="gather_solve",
    )(basis, image, selection)


def rotate_kernel(w_ref, q_ref, c_ref, o_ref, both):
    @pl.when(pl.program_id(1) == 0)
    def _():
        both[...] = jnp.zeros_like(both)
        both[:KEPT, :COLS] = c_ref[0]
        both[KEPT:, COLS:] = c_ref[0]

    rows = jnp.concatenate([w_ref[0], q_ref[0]], axis=1)
    o_ref[0] = lax.dot_general(
        rows, both[...], (((1,), (1,)), ((), ())), preferred_element_type=F32
    ).astype(BF16)


def rotated(basis, image, coeffs):
    block = 2048
    data = pl.BlockSpec((1, block, COLS), lambda s, i: (s, i, 0))
    return pl.pallas_call(
        rotate_kernel,
        grid=(SYSTEMS, DEPTH // block),
        out_shape=jax.ShapeDtypeStruct((SYSTEMS, DEPTH, COLS), BF16),
        in_specs=[data, data, pl.BlockSpec((1, KEPT, COLS), lambda s, i: (s, 0, 0))],
        out_specs=data,
        scratch_shapes=[pltpu.VMEM((2 * KEPT, 2 * COLS), BF16)],
        name="rotate",
    )(basis, image, coeffs)


def on_device(basis, image, selection):
    total_rows = basis.shape[1] * lax.axis_size("rows") * lax.axis_size("groups")
    coeffs = gathered(basis, image, selection, total_rows)
    return rotated(basis, image, coeffs)


def solution(mesh):
    in_specs = (P(None, ("rows", "groups"), None), P(None, ("rows", "groups"), None), P())
    out_specs = P(None, ("rows", "groups"), None)
    return jax.shard_map(
        on_device, mesh=mesh, in_specs=in_specs, out_specs=out_specs, check_vma=False
    )
```

```python
import functools

import jax
import jax.numpy as jnp
from jax import lax
from jax.experimental import pallas as pl
from jax.experimental.pallas import tpu as pltpu
from jax.sharding import PartitionSpec as P

ITERS = 3
F32 = jnp.float32
BF16 = jnp.bfloat16
SYSTEMS = 8
DEPTH = 4096
COLS = 128
KEPT = 64
CHIPS = 64
PLANE = 16


def split(a):
    high = a.astype(BF16)
    rest = a - high.astype(F32)
    middle = rest.astype(BF16)
    return high, middle, (rest - middle.astype(F32)).astype(BF16)


def dot(a, b, over_a, over_b):
    dims = (((over_a,), (over_b,)), ((), ()))

    def both(p, q, r, s):
        return lax.dot_general(
            jnp.concatenate([p, q], axis=over_a), jnp.concatenate([r, s], axis=over_b), dims,
            preferred_element_type=F32,
        )

    (a1, a2, a3), (b1, b2, b3) = split(a), split(b)
    return both(a1, a2, b1, b1) + (both(a1, a2, b2, b2) + both(a1, a3, b3, b1))


def lane(tile, j):
    return jnp.broadcast_to(tile[:, j : j + 1], (8, 128))


def row(tile, j):
    return jnp.broadcast_to(tile[j : j + 1, :], (8, 128))


def added(parts):
    while len(parts) > 1:
        parts = [parts[i] + parts[i + 1] for i in range(0, len(parts), 2)]
    return parts[0]


def times(cols, tile):
    return added([cols[j] * row(tile, j) for j in range(8)])


def less(tile, cols, rows):
    return tile - added([cols[j] * rows[j] for j in range(8)])


def pivot(v, j, at, r):
    piv = v[j]
    for other in range(8):
        if other != j:
            w = row(v[other], j) * r
            v[other] = jnp.where(at, w, v[other] - piv * w)
    v[j] = jnp.where(at, r, -(piv * r))


def stacked(parts):
    return jnp.concatenate(parts, axis=0)


def tiles(a):
    return [a[8 * i : 8 * i + 8] for i in range(a.shape[0] // 8)]


def gauss_jordan(f, x, start, sub):
    for k in range(8):
        v = [lane(f[k], start + 8 * k + j) + 0.0 for j in range(8)]
        cols = {
            i: [lane(f[i], start + 8 * k + j) for j in range(8)]
            for i in [*range(k + 1, 8), *range(k)]
        }
        for j in range(8):
            pivot(v, j, sub == j, 1.0 / row(v[j], j))
        fk, xk = times(v, f[k]), times(v, x[k])
        fr = [row(fk, j) for j in range(8)]
        xr = [row(xk, j) for j in range(8)]
        for i in cols:
            f[i] = less(f[i], cols[i], fr)
            x[i] = less(x[i], cols[i], xr)
        f[k], x[k] = fk, xk


def solved(f, x, sub):
    half = f.shape[0] // 2
    left = lax.broadcasted_iota(jnp.int32, (half, 128), 1) < half
    zero = jnp.zeros((half, 128), F32)
    low = f[half:]
    ft, xt = tiles(f[:half]), tiles(x[:half])
    gauss_jordan(ft, xt, 0, sub)
    ft, xt = stacked(ft), stacked(xt)
    right = jnp.concatenate([stacked([ft, zero]), stacked([xt, zero])], axis=1)
    step = dot(jnp.where(left, low, 0.0), right, 1, 0)
    fl, xl = tiles(low - step[:, :128]), tiles(x[half:] - step[:, 128:])
    gauss_jordan(fl, xl, half, sub)
    xl = stacked(xl)
    return stacked([xt - dot(jnp.where(left, 0.0, ft), stacked([zero, xl]), 1, 0), xl])


def normalised_rows(m, y, sub):
    n = len(m)
    out = []
    for k in range(n):
        v = [lane(m[k], 8 * k + j) + 0.0 for j in range(8)]
        cols = {i: [lane(m[i], 8 * k + j) for j in range(8)] for i in range(k + 1, n)}
        mine = y[k]
        scale = jnp.zeros((8, 128), F32)
        for j in range(8):
            p = row(v[j], j)
            r = 1.0 / p
            at = sub == j
            scale = jnp.where(at, p, scale)
            mine = mine - jnp.where(sub > j, v[j] * r, 0.0) * row(mine, j)
            pivot(v, j, at, r)
        out.append(mine * lax.rsqrt(scale))
        if k < n - 1:
            mk, yk = times(v, m[k]), times(v, y[k])
            mr = [row(mk, j) for j in range(8)]
            yr = [row(yk, j) for j in range(8)]
            for i in cols:
                m[i] = less(m[i], cols[i], mr)
                y[i] = less(y[i], cols[i], yr)
    return out


def system_at(step, x, core):
    hop = (2, 1, 3, 0)[step // 2]
    return 2 * lax.rem(x + hop, 4) + (1 - core if step % 2 == 0 else core)


def gather_kernel(
    total_rows, w_hbm, q_hbm, chosen_hbm, out_ref, wq,
    chosen_ref, lent, given, sums, arrived, diagonals, pieces, coeffs, local_coeffs,
    load_sem, lent_sem, given_sem, send_sem, recv_sem, diag_send, diag_recv,
    share_send, share_recv, share_diag_send, share_diag_recv, done_send, done_recv, chosen_sem,
):
    me_row, me_group = lax.axis_index("rows"), lax.axis_index("groups")
    x, core = me_group // 2, lax.rem(me_group, 2)
    y, z = me_row // 4, lax.rem(me_row, 4)
    xs, ys, zs = ([lax.rem(c + d, 4) for d in range(4)] for c in (x, y, z))
    row_at = [4 * ys[j // 4] + zs[j % 4] for j in range(PLANE)]
    to_first = 4 * lax.rem(4 - y, 4) + lax.rem(4 - z, 4)

    def device(rows, groups):
        return dict(
            device_id={"rows": rows, "groups": groups}, device_id_type=pl.DeviceIdType.MESH
        )

    def landed(ref, sem):
        pltpu.make_async_copy(ref, ref, sem).wait()

    def load(step):
        s = system_at(step, x, core)
        return [
            pltpu.make_async_copy(ref.at[s], wq.at[step, :, pl.ds(off, COLS)], load_sem.at[step, i])
            for i, (ref, off) in enumerate(((w_hbm, 0), (q_hbm, COLS)))
        ]

    ahead = 4
    for step in range(ahead):
        for copy in load(step):
            copy.start()
    fetch_chosen = pltpu.make_async_copy(chosen_hbm, chosen_ref, chosen_sem)
    fetch_chosen.start()

    barrier = pltpu.get_barrier_semaphore()
    for hop in range(4):
        pl.semaphore_signal(barrier, inc=1, **device(me_row, 2 * xs[hop] + 1 - core))
        for j in range(PLANE):
            if hop or j:
                pl.semaphore_signal(barrier, inc=1, **device(row_at[j], 2 * xs[hop] + core))

    across = lax.broadcasted_iota(jnp.int32, (COLS, COLS), 1)
    down = lax.broadcasted_iota(jnp.int32, (COLS, COLS), 0)

    def gram(step, ref):
        for copy in load(step):
            copy.wait()
        over_rows = (((0,), (0,)), ((), ()))
        w, q = wq[step, :, :COLS], wq[step, :, COLS:]
        gram_s = lax.dot_general(w, w, over_rows, preferred_element_type=F32)
        g = lax.dot_general(q, wq[step], over_rows, preferred_element_type=F32)
        gram_f = g[:, COLS:]
        ref[pl.ds(0, PLANE), 0:8, :] = g[:, :COLS].reshape(PLANE, 8, COLS)
        ref[pl.ds(0, PLANE), 8:16, :] = jnp.where(down >= across, gram_s, gram_f).reshape(
            PLANE, 8, COLS
        )
        diagonal = jnp.sum(jnp.where(down == across, gram_f, 0.0), axis=0, keepdims=True)
        ref[PLANE] = jnp.broadcast_to(diagonal, (16, COLS))
        if step + ahead < SYSTEMS:
            for copy in load(step + ahead):
                copy.start()

    def lend(k):
        return pltpu.make_async_remote_copy(
            src_ref=lent.at[k], dst_ref=given.at[k], send_sem=lent_sem.at[k],
            recv_sem=given_sem.at[k], **device(me_row, 2 * x + 1 - core),
        )

    def scatter(k):
        hop = (2, 1, 3, 0)[k]
        target = 2 * xs[hop] + core
        for j in range(PLANE):
            if hop or j:
                pltpu.make_async_remote_copy(
                    src_ref=sums.at[k, row_at[j]], dst_ref=arrived.at[PLANE * hop + j],
                    send_sem=send_sem, recv_sem=recv_sem, **device(row_at[j], target),
                ).start()

        def diagonal():
            pltpu.make_async_remote_copy(
                src_ref=sums.at[k, PLANE, pl.ds(0, 8)], dst_ref=diagonals.at[PLANE * hop + to_first],
                send_sem=diag_send, recv_sem=diag_recv, **device(0, target),
            ).start()

        if hop:
            diagonal()
        else:
            pl.when(me_row != 0)(diagonal)
            arrived[0] = sums[k, me_row]

            @pl.when(me_row == 0)
            def _():
                diagonals[0] = sums[k, PLANE, 0:8]

    gram(0, lent.at[0])
    pl.semaphore_wait(barrier, CHIPS - 1 + 4)
    lend(0).start()
    for k in range(4):
        gram(2 * k + 1, sums.at[k])
        if k < 3:
            gram(2 * k + 2, lent.at[k + 1])
            lend(k + 1).start()
        lend(k).wait_recv()
        sums[k] = sums[k] + given[k]
        scatter(k)

    fetch_chosen.wait()
    chosen = chosen_ref[pl.ds(me_group, 1), :]
    coeffs[...] = (lax.broadcasted_iota(jnp.int32, (COLS, KEPT), 0) == chosen).astype(F32).T

    others = arrived.at[pl.ds(1, CHIPS - 1)]
    landed(others, recv_sem)

    def add(i, total):
        return total + arrived[i]

    pieces[me_row] = lax.fori_loop(1, CHIPS, add, arrived[0], unroll=9)

    def share(j, part, send, recv):
        return pltpu.make_async_remote_copy(
            src_ref=part, dst_ref=part, send_sem=send, recv_sem=recv, **device(row_at[j], me_group)
        )

    for j in range(1, PLANE):
        share(j, pieces.at[me_row], share_send, share_recv).start()
    fifteen = pieces.at[pl.ds(0, PLANE - 1)]
    shared_diagonal = pieces.at[PLANE, pl.ds(0, 8)]

    @pl.when(me_row == 0)
    def _():
        landed(diagonals.at[pl.ds(1, CHIPS - 1)], diag_recv)
        pieces[PLANE, 0:8, :] = lax.fori_loop(
            1, CHIPS, lambda i, total: total + diagonals[i], diagonals[0], unroll=9
        )
        for j in range(1, PLANE):
            share(j, shared_diagonal, share_diag_send, share_diag_recv).start()

    @pl.when(me_row != 0)
    def _():
        landed(shared_diagonal, share_diag_recv)

    landed(fifteen, share_recv)

    sub = lax.broadcasted_iota(jnp.int32, (8, 128), 0)
    mixed = stacked([pieces[i, 8:16, :] for i in range(PLANE)])
    turned = mixed.T
    diagonal = jnp.broadcast_to(pieces[PLANE, 0:1, :], (COLS, COLS))
    gram_f = jnp.where(down < across, mixed, jnp.where(down == across, diagonal, turned))
    gram_s = jnp.where(down >= across, mixed, turned)
    step_matrix = solved(gram_f, stacked([pieces[i, 0:8, :] for i in range(PLANE)]), sub)
    moves = stacked([step_matrix, dot(gram_s, step_matrix, 1, 0)])

    def iterate(i, _):
        moved = dot(coeffs[...], moves, 1, 1)
        solution_t, weighted = moved[:, :COLS], moved[:, COLS:]
        metric = dot(solution_t, weighted, 1, 1) * (1.0 / total_rows)
        wide = jnp.concatenate([metric, jnp.zeros((KEPT, COLS - KEPT), F32)], axis=1)
        coeffs[...] = stacked(normalised_rows(tiles(wide), tiles(solution_t), sub))
        return 0

    lax.fori_loop(0, ITERS, iterate, 0)
    local_coeffs[...] = coeffs[...].astype(BF16)
    out_ref[me_group] = local_coeffs[...]
    for i in range(1, SYSTEMS):
        pltpu.make_async_remote_copy(
            src_ref=local_coeffs, dst_ref=out_ref.at[me_group], send_sem=done_send,
            recv_sem=done_recv, **device(me_row, lax.rem(me_group + i, SYSTEMS)),
        ).start()
    seven = out_ref.at[pl.ds(0, SYSTEMS - 1)]
    landed(seven, done_recv)
    landed(seven, done_send)
    landed(fifteen, share_send)
    landed(others, send_sem)
    landed(diagonals.at[pl.ds(0, 3)], diag_send)

    @pl.when(me_row != 0)
    def _():
        landed(shared_diagonal, diag_send)

    @pl.when(me_row == 0)
    def _():
        landed(diagonals.at[pl.ds(0, PLANE - 1)], share_diag_send)

    for k in range(4):
        lend(k).wait_send()


def in_hbm(a):
    return pltpu.with_memory_space_constraint(a, pltpu.HBM)


def gathered(basis, image, selection, total_rows):
    piece = (16, COLS)
    dma = pltpu.SemaphoreType.DMA
    return pl.pallas_call(
        functools.partial(gather_kernel, total_rows),
        out_shape=[
            pltpu.VMEM((SYSTEMS, KEPT, COLS), BF16),
            pltpu.VMEM((SYSTEMS, DEPTH, 2 * COLS), BF16),
        ],
        in_specs=[pl.BlockSpec(memory_space=pltpu.HBM)] * 3,
        out_specs=[pl.BlockSpec(memory_space=pltpu.VMEM)] * 2,
        scratch_shapes=[
            pltpu.VMEM((SYSTEMS, KEPT), jnp.int32),
            pltpu.VMEM((4, PLANE + 1, *piece), F32),
            pltpu.VMEM((4, PLANE + 1, *piece), F32),
            pltpu.VMEM((4, PLANE + 1, *piece), F32),
            pltpu.VMEM((CHIPS, *piece), F32),
            pltpu.VMEM((CHIPS, 8, COLS), F32),
            pltpu.VMEM((PLANE + 1, *piece), F32),
            pltpu.VMEM((KEPT, COLS), F32),
            pltpu.VMEM((KEPT, COLS), BF16),
            dma((SYSTEMS, 2)),
            dma((4,)),
            dma((4,)),
            *[dma] * 11,
        ],
        compiler_params=pltpu.CompilerParams(
            collective_id=0, has_side_effects=True, vmem_limit_bytes=40 * 2**20
        ),
        name="gather_solve",
    )(in_hbm(basis), in_hbm(image), in_hbm(selection))


def rotate_kernel(wq, c_ref, o_hbm, both, out, sem):
    group = lax.axis_index("groups")
    x, core = group // 2, lax.rem(group, 2)
    block, part = out.shape[1], 512
    per = DEPTH // block
    both[...] = jnp.zeros_like(both)

    def store(t):
        s = system_at(t // per, x, core)
        return pltpu.make_async_copy(
            out.at[t], o_hbm.at[s, pl.ds(t % per * block, block)], sem.at[t]
        )

    for t in range(SYSTEMS * per):
        step, slot = t // per, t // per % 2
        if t % per == 0:
            coeffs = c_ref[system_at(step, x, core)]
            both[slot, :KEPT, :COLS] = coeffs
            both[slot, KEPT:, COLS:] = coeffs
        for u in range(0, block, part):
            at = t % per * block + u
            out[t, u : u + part] = lax.dot_general(
                wq[step, at : at + part, :], both[slot],
                (((1,), (1,)), ((), ())), preferred_element_type=F32,
            ).astype(BF16)
        store(t).start()
    for t in range(SYSTEMS * per):
        store(t).wait()


def rotated(wq, coeffs):
    block = 2048
    blocks = SYSTEMS * DEPTH // block
    return pl.pallas_call(
        rotate_kernel,
        out_shape=jax.ShapeDtypeStruct((SYSTEMS, DEPTH, COLS), BF16),
        in_specs=[pl.BlockSpec(memory_space=pltpu.VMEM)] * 2,
        out_specs=pl.BlockSpec(memory_space=pltpu.HBM),
        scratch_shapes=[
            pltpu.VMEM((2, 2 * KEPT, 2 * COLS), BF16),
            pltpu.VMEM((blocks, block, COLS), BF16),
            pltpu.SemaphoreType.DMA((blocks,)),
        ],
        compiler_params=pltpu.CompilerParams(vmem_limit_bytes=24 * 2**20),
        name="rotate",
    )(wq, coeffs)


def on_device(basis, image, selection):
    total_rows = basis.shape[1] * lax.axis_size("rows") * lax.axis_size("groups")
    coeffs, wq = gathered(basis, image, selection, total_rows)
    return rotated(wq, coeffs)


def solution(mesh):
    in_specs = (P(None, ("rows", "groups"), None), P(None, ("rows", "groups"), None), P())
    out_specs = P(None, ("rows", "groups"), None)
    return jax.shard_map(
        on_device, mesh=mesh, in_specs=in_specs, out_specs=out_specs, check_vma=False
    )
```

```python
import functools

import jax
import jax.numpy as jnp
from jax import lax
from jax.experimental import pallas as pl
from jax.experimental.pallas import tpu as pltpu
from jax.sharding import PartitionSpec as P

ITERS = 3
EARLY = 1
TURNED = 4
F32 = jnp.float32
BF16 = jnp.bfloat16
SYSTEMS = 8
DEPTH = 4096
COLS = 128
KEPT = 64
CHIPS = 64
PLANE = 16


def split(a):
    high = a.astype(BF16)
    rest = a - high.astype(F32)
    middle = rest.astype(BF16)
    return high, middle, (rest - middle.astype(F32)).astype(BF16)


def dot(a, b, over_a, over_b):
    dims = (((over_a,), (over_b,)), ((), ()))

    def both(p, q, r, s):
        return lax.dot_general(
            jnp.concatenate([p, q], axis=over_a), jnp.concatenate([r, s], axis=over_b), dims,
            preferred_element_type=F32,
        )

    (a1, a2, a3), (b1, b2, b3) = split(a), split(b)
    return both(a1, a2, b1, b1) + (both(a1, a2, b2, b2) + both(a1, a3, b3, b1))


def lane(tile, j):
    return jnp.broadcast_to(tile[:, j : j + 1], (8, 128))


def row(tile, j):
    return jnp.broadcast_to(tile[j : j + 1, :], (8, 128))


def added(parts):
    while len(parts) > 1:
        parts = [parts[i] + parts[i + 1] for i in range(0, len(parts), 2)]
    return parts[0]


def times(cols, tile):
    return added([cols[j] * row(tile, j) for j in range(8)])


def less(tile, cols, rows):
    return tile - added([cols[j] * rows[j] for j in range(8)])


def pivot_pair(v, j, sub):
    at, at_next = sub == j, sub == j + 1
    a, b1, b2, c = row(v[j], j), row(v[j + 1], j), row(v[j], j + 1), row(v[j + 1], j + 1)
    r = 1.0 / (a * c - b1 * b2)
    p = jnp.where(at, -1.0, jnp.where(at_next, 0.0, v[j]))
    q = jnp.where(at_next, -1.0, jnp.where(at, 0.0, v[j + 1]))
    v[j], v[j + 1] = r * (q * b2 - p * c), r * (p * b1 - q * a)
    for other in range(8):
        if other not in (j, j + 1):
            u, t = row(v[other], j), row(v[other], j + 1)
            moved = p * (c * u - b1 * t) + q * (a * t - b2 * u)
            v[other] = jnp.where(at | at_next, 0.0, v[other]) - r * moved
    return a, b1, b2, c, r


def stacked(parts):
    return jnp.concatenate(parts, axis=0)


def tiles(a):
    return [a[8 * i : 8 * i + 8] for i in range(a.shape[0] // 8)]


def gauss_jordan(f, x, start, sub):
    for k in range(8):
        v = [lane(f[k], start + 8 * k + j) + 0.0 for j in range(8)]
        cols = {
            i: [lane(f[i], start + 8 * k + j) for j in range(8)]
            for i in [*range(k + 1, 8), *range(k)]
        }
        for j in range(0, 8, 2):
            pivot_pair(v, j, sub)
        fk, xk = times(v, f[k]), times(v, x[k])
        fr = [row(fk, j) for j in range(8)]
        xr = [row(xk, j) for j in range(8)]
        for i in cols:
            f[i] = less(f[i], cols[i], fr)
            x[i] = less(x[i], cols[i], xr)
        f[k], x[k] = fk, xk


def solved(f, x, sub):
    half = f.shape[0] // 2
    left = lax.broadcasted_iota(jnp.int32, (half, 128), 1) < half
    zero = jnp.zeros((half, 128), F32)
    low = f[half:]
    ft, xt = tiles(f[:half]), tiles(x[:half])
    gauss_jordan(ft, xt, 0, sub)
    ft, xt = stacked(ft), stacked(xt)
    right = jnp.concatenate([stacked([ft, zero]), stacked([xt, zero])], axis=1)
    step = dot(jnp.where(left, low, 0.0), right, 1, 0)
    fl, xl = tiles(low - step[:, :128]), tiles(x[half:] - step[:, 128:])
    gauss_jordan(fl, xl, half, sub)
    xl = stacked(xl)
    return stacked([xt - dot(jnp.where(left, 0.0, ft), stacked([zero, xl]), 1, 0), xl])


def normalised_rows(m, y, sub):
    n = len(m)
    out = []
    for k in range(n):
        v = [lane(m[k], 8 * k + j) + 0.0 for j in range(8)]
        cols = {i: [lane(m[i], 8 * k + j) for j in range(8)] for i in range(k + 1, n)}
        mine = y[k]
        scale = jnp.zeros((8, 128), F32)
        for j in range(0, 8, 2):
            p, q = v[j], v[j + 1]
            a, b1, b2, c, r = pivot_pair(v, j, sub)
            inverse_a = 1.0 / a
            g, h = row(mine, j), row(mine, j + 1)
            below = r * (p * (c * g - b1 * h) + q * (a * h - b2 * g))
            mine = mine - jnp.where(
                sub > j + 1, below, jnp.where(sub == j + 1, (b2 * inverse_a) * g, 0.0)
            )
            second = (a * c - b1 * b2) * inverse_a
            scale = jnp.where(sub == j, a, jnp.where(sub == j + 1, second, scale))
        out.append(mine * lax.rsqrt(scale))
        if k < n - 1:
            mk, yk = times(v, m[k]), times(v, y[k])
            mr = [row(mk, j) for j in range(8)]
            yr = [row(yk, j) for j in range(8)]
            for i in cols:
                m[i] = less(m[i], cols[i], mr)
                y[i] = less(y[i], cols[i], yr)
    return out


def unit_scale(m):
    on = lax.broadcasted_iota(jnp.int32, m.shape, 0) == lax.broadcasted_iota(jnp.int32, m.shape, 1)
    diagonal = jnp.where(on, m, 0.0)
    return [lax.rsqrt(jnp.sum(diagonal, axis=axis, keepdims=True)) for axis in (1, 0)]


def system_at(step, x, core):
    hop = (2, 1, 3, 0)[step // 2]
    return 2 * lax.rem(x + hop, 4) + (1 - core if step % 2 == 0 else core)


ROTATION_ORDER = (7, 6, 5, 4, 3, 2, 1, 0)


def rotate(both, coeffs, data, out):
    part = 512
    both[:KEPT, :COLS] = coeffs
    both[KEPT:, COLS:] = coeffs
    for at in range(0, DEPTH, part):
        out[at : at + part] = lax.dot_general(
            data[at : at + part], both[...], (((1,), (1,)), ((), ())), preferred_element_type=F32
        ).astype(BF16)


def gather_kernel(
    total_rows, w_hbm, q_hbm, chosen_hbm, out_ref, wq, turned,
    both, chosen_ref, lent, given, sums, arrived, diagonals, pieces, coeffs, local_coeffs,
    load_sem, lent_sem, given_sem, send_sem, recv_sem, diag_send, diag_recv,
    share_send, share_recv, share_diag_send, share_diag_recv, done_send, done_recv, chosen_sem,
):
    me_row, me_group = lax.axis_index("rows"), lax.axis_index("groups")
    x, core = me_group // 2, lax.rem(me_group, 2)
    y, z = me_row // 4, lax.rem(me_row, 4)
    xs, ys, zs = ([lax.rem(c + d, 4) for d in range(4)] for c in (x, y, z))
    row_at = [4 * ys[j // 4] + zs[j % 4] for j in range(PLANE)]
    to_first = 4 * lax.rem(4 - y, 4) + lax.rem(4 - z, 4)

    def device(rows, groups):
        return dict(
            device_id={"rows": rows, "groups": groups}, device_id_type=pl.DeviceIdType.MESH
        )

    def landed(ref, sem):
        pltpu.make_async_copy(ref, ref, sem).wait()

    def load(step):
        s = system_at(step, x, core)
        return [
            pltpu.make_async_copy(ref.at[s], wq.at[step, :, pl.ds(off, COLS)], load_sem.at[step, i])
            for i, (ref, off) in enumerate(((w_hbm, 0), (q_hbm, COLS)))
        ]

    ahead = 4
    for step in range(ahead):
        for copy in load(step):
            copy.start()
    fetch_chosen = pltpu.make_async_copy(chosen_hbm, chosen_ref, chosen_sem)
    fetch_chosen.start()

    barrier = pltpu.get_barrier_semaphore()
    for hop in range(4):
        pl.semaphore_signal(barrier, inc=1, **device(me_row, 2 * xs[hop] + 1 - core))
        for j in range(PLANE):
            if hop or j:
                pl.semaphore_signal(barrier, inc=1, **device(row_at[j], 2 * xs[hop] + core))

    across = lax.broadcasted_iota(jnp.int32, (COLS, COLS), 1)
    down = lax.broadcasted_iota(jnp.int32, (COLS, COLS), 0)

    def gram(step, ref):
        for copy in load(step):
            copy.wait()
        over_rows = (((0,), (0,)), ((), ()))
        w, q = wq[step, :, :COLS], wq[step, :, COLS:]
        gram_s = lax.dot_general(w, w, over_rows, preferred_element_type=F32)
        g = lax.dot_general(q, wq[step], over_rows, preferred_element_type=F32)
        gram_f = g[:, COLS:]
        ref[pl.ds(0, PLANE), 0:8, :] = g[:, :COLS].reshape(PLANE, 8, COLS)
        ref[pl.ds(0, PLANE), 8:16, :] = jnp.where(down >= across, gram_s, gram_f).reshape(
            PLANE, 8, COLS
        )
        diagonal = jnp.sum(jnp.where(down == across, gram_f, 0.0), axis=0, keepdims=True)
        ref[PLANE] = jnp.broadcast_to(diagonal, (16, COLS))
        if step + ahead < SYSTEMS:
            for copy in load(step + ahead):
                copy.start()

    def lend(k):
        return pltpu.make_async_remote_copy(
            src_ref=lent.at[k], dst_ref=given.at[k], send_sem=lent_sem.at[k],
            recv_sem=given_sem.at[k], **device(me_row, 2 * x + 1 - core),
        )

    def scatter(k):
        hop = (2, 1, 3, 0)[k]
        target = 2 * xs[hop] + core
        for j in range(PLANE):
            if hop or j:
                pltpu.make_async_remote_copy(
                    src_ref=sums.at[k, row_at[j]], dst_ref=arrived.at[PLANE * hop + j],
                    send_sem=send_sem, recv_sem=recv_sem, **device(row_at[j], target),
                ).start()

        def diagonal():
            pltpu.make_async_remote_copy(
                src_ref=sums.at[k, PLANE, pl.ds(0, 8)], dst_ref=diagonals.at[PLANE * hop + to_first],
                send_sem=diag_send, recv_sem=diag_recv, **device(0, target),
            ).start()

        if hop:
            diagonal()
        else:
            pl.when(me_row != 0)(diagonal)
            arrived[0] = sums[k, me_row]

            @pl.when(me_row == 0)
            def _():
                diagonals[0] = sums[k, PLANE, 0:8]

    def partial_gram(step):
        gram(step, (lent if step % 2 == 0 else sums).at[step // 2])

    def combine(k):
        lend(k).wait_recv()
        sums[k] = sums[k] + given[k]
        scatter(k)

    for step in range(EARLY):
        partial_gram(step)
    pl.semaphore_wait(barrier, CHIPS - 1 + 4)
    lent_out = combined = 0
    for step in range(EARLY, SYSTEMS + 1):
        while 2 * lent_out < step:
            lend(lent_out).start()
            lent_out += 1
        if step < SYSTEMS:
            partial_gram(step)
        while 2 * combined + 1 < step:
            combine(combined)
            combined += 1

    fetch_chosen.wait()
    chosen = chosen_ref[pl.ds(me_group, 1), :]
    coeffs[...] = (lax.broadcasted_iota(jnp.int32, (COLS, KEPT), 0) == chosen).astype(F32).T

    others = arrived.at[pl.ds(1, CHIPS - 1)]
    landed(others, recv_sem)

    def add(i, total):
        return total + arrived[i]

    pieces[me_row] = lax.fori_loop(1, CHIPS, add, arrived[0], unroll=9)

    def share(j, part, send, recv):
        return pltpu.make_async_remote_copy(
            src_ref=part, dst_ref=part, send_sem=send, recv_sem=recv, **device(row_at[j], me_group)
        )

    for j in range(1, PLANE):
        share(j, pieces.at[me_row], share_send, share_recv).start()
    fifteen = pieces.at[pl.ds(0, PLANE - 1)]
    shared_diagonal = pieces.at[PLANE, pl.ds(0, 8)]

    @pl.when(me_row == 0)
    def _():
        landed(diagonals.at[pl.ds(1, CHIPS - 1)], diag_recv)
        pieces[PLANE, 0:8, :] = lax.fori_loop(
            1, CHIPS, lambda i, total: total + diagonals[i], diagonals[0], unroll=9
        )
        for j in range(1, PLANE):
            share(j, shared_diagonal, share_diag_send, share_diag_recv).start()

    @pl.when(me_row != 0)
    def _():
        landed(shared_diagonal, share_diag_recv)

    landed(fifteen, share_recv)

    sub = lax.broadcasted_iota(jnp.int32, (8, 128), 0)
    mixed = stacked([pieces[i, 8:16, :] for i in range(PLANE)])
    mixed_t = mixed.T
    diagonal = jnp.broadcast_to(pieces[PLANE, 0:1, :], (COLS, COLS))
    gram_f = jnp.where(down < across, mixed, jnp.where(down == across, diagonal, mixed_t))
    gram_s = jnp.where(down >= across, mixed, mixed_t)
    by_row, by_col = unit_scale(gram_f)
    cross_t = stacked([pieces[i, 0:8, :] for i in range(PLANE)])
    step_matrix = solved(gram_f * by_row * by_col, cross_t * by_row, sub) * by_row
    moves = stacked([step_matrix, dot(gram_s, step_matrix, 1, 0)])

    def iterate(i, _):
        moved = dot(coeffs[...], moves, 1, 1)
        solution_t, weighted = moved[:, :COLS], moved[:, COLS:]
        metric = dot(solution_t, weighted, 1, 1) * (1.0 / total_rows)
        by_row, by_col = unit_scale(metric)
        metric = metric * by_row * by_col
        wide = jnp.concatenate([metric, jnp.zeros((KEPT, COLS - KEPT), F32)], axis=1)
        coeffs[...] = stacked(normalised_rows(tiles(wide), tiles(solution_t * by_row), sub))
        return 0

    lax.fori_loop(0, ITERS, iterate, 0)
    local_coeffs[...] = coeffs[...].astype(BF16)
    out_ref[me_group] = local_coeffs[...]
    both[...] = jnp.zeros_like(both)

    def tell(hop, same):
        target = 2 * xs[hop] + (core if same else 1 - core)
        return pltpu.make_async_remote_copy(
            src_ref=local_coeffs, dst_ref=out_ref.at[me_group], send_sem=done_send,
            recv_sem=done_recv.at[2 * hop + same], **device(me_row, target),
        )

    for hop, same in ((2, 1), (2, 0), (1, 1), (1, 0), (3, 1), (3, 0), (0, 0)):
        tell(hop, same).start()
    for i, step in enumerate(ROTATION_ORDER):
        hop, same = (2, 1, 3, 0)[step // 2], step % 2
        s = system_at(step, x, core)
        if step != 7:
            landed(out_ref.at[s], done_recv.at[2 * ((4 - hop) % 4) + same])
        if i < TURNED:
            rotate(both.at[i % 2], out_ref[s], wq.at[step], turned.at[i])
    landed(out_ref.at[pl.ds(0, SYSTEMS - 1)], done_send)
    landed(fifteen, share_send)
    landed(others, send_sem)
    landed(diagonals.at[pl.ds(0, 3)], diag_send)

    @pl.when(me_row != 0)
    def _():
        landed(shared_diagonal, diag_send)

    @pl.when(me_row == 0)
    def _():
        landed(diagonals.at[pl.ds(0, PLANE - 1)], share_diag_send)

    for k in range(4):
        lend(k).wait_send()


def in_hbm(a):
    return pltpu.with_memory_space_constraint(a, pltpu.HBM)


def gathered(basis, image, selection, total_rows):
    piece = (16, COLS)
    dma = pltpu.SemaphoreType.DMA
    return pl.pallas_call(
        functools.partial(gather_kernel, total_rows),
        out_shape=[
            pltpu.VMEM((SYSTEMS, KEPT, COLS), BF16),
            pltpu.VMEM((SYSTEMS, DEPTH, 2 * COLS), BF16),
            pltpu.VMEM((TURNED, DEPTH, COLS), BF16),
        ],
        in_specs=[pl.BlockSpec(memory_space=pltpu.HBM)] * 3,
        out_specs=[pl.BlockSpec(memory_space=pltpu.VMEM)] * 3,
        scratch_shapes=[
            pltpu.VMEM((2, 2 * KEPT, 2 * COLS), BF16),
            pltpu.VMEM((SYSTEMS, KEPT), jnp.int32),
            pltpu.VMEM((4, PLANE + 1, *piece), F32),
            pltpu.VMEM((4, PLANE + 1, *piece), F32),
            pltpu.VMEM((4, PLANE + 1, *piece), F32),
            pltpu.VMEM((CHIPS, *piece), F32),
            pltpu.VMEM((CHIPS, 8, COLS), F32),
            pltpu.VMEM((PLANE + 1, *piece), F32),
            pltpu.VMEM((KEPT, COLS), F32),
            pltpu.VMEM((KEPT, COLS), BF16),
            dma((SYSTEMS, 2)),
            dma((4,)),
            dma((4,)),
            *[dma] * 9,
            dma((SYSTEMS,)),
            dma,
        ],
        compiler_params=pltpu.CompilerParams(
            collective_id=0, has_side_effects=True, vmem_limit_bytes=16 * 2**20
        ),
        name="gather_solve",
    )(in_hbm(basis), in_hbm(image), in_hbm(selection))


def rotate_kernel(wq, turned, c_ref, o_hbm, both, out, sem):
    group = lax.axis_index("groups")
    x, core = group // 2, lax.rem(group, 2)

    def store(i):
        source = turned.at[i] if i < TURNED else out.at[i - TURNED]
        return pltpu.make_async_copy(
            source, o_hbm.at[system_at(ROTATION_ORDER[i], x, core)], sem.at[i]
        )

    for i in range(TURNED):
        store(i).start()
    both[...] = jnp.zeros_like(both)
    for i in range(TURNED, SYSTEMS):
        step = ROTATION_ORDER[i]
        coeffs = c_ref[system_at(step, x, core)]
        rotate(both.at[i % 2], coeffs, wq.at[step], out.at[i - TURNED])
        store(i).start()
    for i in range(SYSTEMS):
        store(i).wait()


def rotated(coeffs, wq, turned):
    return pl.pallas_call(
        rotate_kernel,
        out_shape=jax.ShapeDtypeStruct((SYSTEMS, DEPTH, COLS), BF16),
        in_specs=[pl.BlockSpec(memory_space=pltpu.VMEM)] * 3,
        out_specs=pl.BlockSpec(memory_space=pltpu.HBM),
        scratch_shapes=[
            pltpu.VMEM((2, 2 * KEPT, 2 * COLS), BF16),
            pltpu.VMEM((SYSTEMS - TURNED, DEPTH, COLS), BF16),
            pltpu.SemaphoreType.DMA((SYSTEMS,)),
        ],
        compiler_params=pltpu.CompilerParams(vmem_limit_bytes=16 * 2**20),
        name="rotate",
    )(wq, turned, coeffs)


def on_device(basis, image, selection):
    total_rows = basis.shape[1] * lax.axis_size("rows") * lax.axis_size("groups")
    return rotated(*gathered(basis, image, selection, total_rows))


def solution(mesh):
    in_specs = (P(None, ("rows", "groups"), None), P(None, ("rows", "groups"), None), P())
    out_specs = P(None, ("rows", "groups"), None)
    return jax.shard_map(
        on_device, mesh=mesh, in_specs=in_specs, out_specs=out_specs, check_vma=False
    )
```

```python
import functools

import jax
import jax.numpy as jnp
from jax import lax
from jax.experimental import pallas as pl
from jax.experimental.pallas import tpu as pltpu
from jax.sharding import PartitionSpec as P

ITERS = 3
TURNED = 4
F32 = jnp.float32
BF16 = jnp.bfloat16
SYSTEMS = 8
DEPTH = 4096
COLS = 128
KEPT = 64
PLANE = 16


def split(a):
    high = a.astype(BF16)
    rest = a - high.astype(F32)
    middle = rest.astype(BF16)
    return high, middle, (rest - middle.astype(F32)).astype(BF16)


def dot(a, b, over_a, over_b):
    dims = (((over_a,), (over_b,)), ((), ()))

    def both(p, q, r, s):
        return lax.dot_general(
            jnp.concatenate([p, q], axis=over_a), jnp.concatenate([r, s], axis=over_b), dims,
            preferred_element_type=F32,
        )

    (a1, a2, a3), (b1, b2, b3) = split(a), split(b)
    return both(a1, a2, b1, b1) + (both(a1, a2, b2, b2) + both(a1, a3, b3, b1))


def lane(tile, j):
    return jnp.broadcast_to(tile[:, j : j + 1], (8, 128))


def row(tile, j):
    return jnp.broadcast_to(tile[j : j + 1, :], (8, 128))


def added(parts):
    while len(parts) > 1:
        parts = [parts[i] + parts[i + 1] for i in range(0, len(parts), 2)]
    return parts[0]


def times(cols, tile):
    return added([cols[j] * row(tile, j) for j in range(8)])


def less(tile, cols, rows):
    return tile - added([cols[j] * rows[j] for j in range(8)])


def pivot_pair(v, j, sub):
    at, at_next = sub == j, sub == j + 1
    a, b1, b2, c = row(v[j], j), row(v[j + 1], j), row(v[j], j + 1), row(v[j + 1], j + 1)
    r = 1.0 / (a * c - b1 * b2)
    p = jnp.where(at, -1.0, jnp.where(at_next, 0.0, v[j]))
    q = jnp.where(at_next, -1.0, jnp.where(at, 0.0, v[j + 1]))
    v[j], v[j + 1] = r * (q * b2 - p * c), r * (p * b1 - q * a)
    for other in range(8):
        if other not in (j, j + 1):
            u, t = row(v[other], j), row(v[other], j + 1)
            moved = p * (c * u - b1 * t) + q * (a * t - b2 * u)
            v[other] = jnp.where(at | at_next, 0.0, v[other]) - r * moved
    return a, b1, b2, c, r


def stacked(parts):
    return jnp.concatenate(parts, axis=0)


def tiles(a):
    return [a[8 * i : 8 * i + 8] for i in range(a.shape[0] // 8)]


def gauss_jordan(f, x, start, sub):
    for k in range(8):
        v = [lane(f[k], start + 8 * k + j) + 0.0 for j in range(8)]
        cols = {
            i: [lane(f[i], start + 8 * k + j) for j in range(8)]
            for i in [*range(k + 1, 8), *range(k)]
        }
        for j in range(0, 8, 2):
            pivot_pair(v, j, sub)
        fk, xk = times(v, f[k]), times(v, x[k])
        fr = [row(fk, j) for j in range(8)]
        xr = [row(xk, j) for j in range(8)]
        for i in cols:
            f[i] = less(f[i], cols[i], fr)
            x[i] = less(x[i], cols[i], xr)
        f[k], x[k] = fk, xk


def solved(f, x, sub):
    half = f.shape[0] // 2
    left = lax.broadcasted_iota(jnp.int32, (half, 128), 1) < half
    zero = jnp.zeros((half, 128), F32)
    low = f[half:]
    ft, xt = tiles(f[:half]), tiles(x[:half])
    gauss_jordan(ft, xt, 0, sub)
    ft, xt = stacked(ft), stacked(xt)
    right = jnp.concatenate([stacked([ft, zero]), stacked([xt, zero])], axis=1)
    step = dot(jnp.where(left, low, 0.0), right, 1, 0)
    fl, xl = tiles(low - step[:, :128]), tiles(x[half:] - step[:, 128:])
    gauss_jordan(fl, xl, half, sub)
    xl = stacked(xl)
    return stacked([xt - dot(jnp.where(left, 0.0, ft), stacked([zero, xl]), 1, 0), xl])


def normalised_rows(m, y, sub):
    n = len(m)
    out = []
    for k in range(n):
        v = [lane(m[k], 8 * k + j) + 0.0 for j in range(8)]
        cols = {i: [lane(m[i], 8 * k + j) for j in range(8)] for i in range(k + 1, n)}
        mine = y[k]
        scale = jnp.zeros((8, 128), F32)
        for j in range(0, 8, 2):
            p, q = v[j], v[j + 1]
            a, b1, b2, c, r = pivot_pair(v, j, sub)
            inverse_a = 1.0 / a
            g, h = row(mine, j), row(mine, j + 1)
            below = r * (p * (c * g - b1 * h) + q * (a * h - b2 * g))
            mine = mine - jnp.where(
                sub > j + 1, below, jnp.where(sub == j + 1, (b2 * inverse_a) * g, 0.0)
            )
            second = (a * c - b1 * b2) * inverse_a
            scale = jnp.where(sub == j, a, jnp.where(sub == j + 1, second, scale))
        out.append(mine * lax.rsqrt(scale))
        if k < n - 1:
            mk, yk = times(v, m[k]), times(v, y[k])
            mr = [row(mk, j) for j in range(8)]
            yr = [row(yk, j) for j in range(8)]
            for i in cols:
                m[i] = less(m[i], cols[i], mr)
                y[i] = less(y[i], cols[i], yr)
    return out


def unit_scale(m):
    on = lax.broadcasted_iota(jnp.int32, m.shape, 0) == lax.broadcasted_iota(jnp.int32, m.shape, 1)
    diagonal = jnp.where(on, m, 0.0)
    return [lax.rsqrt(jnp.sum(diagonal, axis=axis, keepdims=True)) for axis in (1, 0)]


HOPS = (2, 0, 1, 3)
ORDER = ((0, 0), (1, 0), (0, 1), (2, 0), (1, 1), (3, 0), (2, 1), (3, 1))
AHEAD = 4
LANDING = {0: 0, 1: 1, 3: 2}
SENDERS = 3 * PLANE


def system_at(step, x, core):
    k, own = ORDER[step]
    return 2 * lax.rem(x + HOPS[k], 4) + (core if own else 1 - core)


ROTATION_ORDER = tuple(ORDER.index(c) for c in ((1, 1), (1, 0), (2, 1), (2, 0), (3, 1), (3, 0), (0, 1), (0, 0)))


def rotate(both, coeffs, data, out):
    part = 512
    both[:KEPT, :COLS] = coeffs
    both[KEPT:, COLS:] = coeffs
    for at in range(0, DEPTH, part):
        out[at : at + part] = lax.dot_general(
            data[at : at + part], both[...], (((1,), (1,)), ((), ())), preferred_element_type=F32
        ).astype(BF16)


def gather_kernel(
    total_rows, w_hbm, q_hbm, chosen_hbm, out_ref, wq, turned,
    both, chosen_ref, lent, given, sums, relayed, arrived, diagonals, pieces, coeffs, local_coeffs,
    load_sem, lent_sem, given_sem, relay_send, relay_recv, send_sem, recv_sem, diag_send, diag_recv,
    share_send, share_recv, share_diag_send, share_diag_recv, done_send, done_recv, chosen_sem,
):
    me_row, me_group = lax.axis_index("rows"), lax.axis_index("groups")
    x, core = me_group // 2, lax.rem(me_group, 2)
    y, z = me_row // 4, lax.rem(me_row, 4)
    xs, ys, zs = ([lax.rem(c + d, 4) for d in range(4)] for c in (x, y, z))
    row_at = [4 * ys[j // 4] + zs[j % 4] for j in range(PLANE)]
    to_first = 4 * lax.rem(4 - y, 4) + lax.rem(4 - z, 4)

    def device(rows, groups):
        return dict(
            device_id={"rows": rows, "groups": groups}, device_id_type=pl.DeviceIdType.MESH
        )

    def landed(ref, sem):
        pltpu.make_async_copy(ref, ref, sem).wait()

    def load(step):
        s = system_at(step, x, core)
        return [
            pltpu.make_async_copy(ref.at[s], wq.at[step, :, pl.ds(off, COLS)], load_sem.at[step, i])
            for i, (ref, off) in enumerate(((w_hbm, 0), (q_hbm, COLS)))
        ]

    for step in range(AHEAD):
        for copy in load(step):
            copy.start()
    fetch_chosen = pltpu.make_async_copy(chosen_hbm, chosen_ref, chosen_sem)
    fetch_chosen.start()

    barrier = pltpu.get_barrier_semaphore()
    for hop in range(4):
        pl.semaphore_signal(barrier, inc=1, **device(me_row, 2 * xs[hop] + 1 - core))
        for j in range(PLANE if hop != 2 else 1):
            if hop or j:
                pl.semaphore_signal(barrier, inc=1, **device(row_at[j], 2 * xs[hop] + core))

    across = lax.broadcasted_iota(jnp.int32, (COLS, COLS), 1)
    down = lax.broadcasted_iota(jnp.int32, (COLS, COLS), 0)

    def gram(step, ref):
        for copy in load(step):
            copy.wait()
        over_rows = (((0,), (0,)), ((), ()))
        w, q = wq[step, :, :COLS], wq[step, :, COLS:]
        gram_s = lax.dot_general(w, w, over_rows, preferred_element_type=F32)
        g = lax.dot_general(q, wq[step], over_rows, preferred_element_type=F32)
        gram_f = g[:, COLS:]
        ref[pl.ds(0, PLANE), 0:8, :] = g[:, :COLS].reshape(PLANE, 8, COLS)
        ref[pl.ds(0, PLANE), 8:16, :] = jnp.where(down >= across, gram_s, gram_f).reshape(
            PLANE, 8, COLS
        )
        diagonal = jnp.sum(jnp.where(down == across, gram_f, 0.0), axis=0, keepdims=True)
        ref[PLANE] = jnp.broadcast_to(diagonal, (16, COLS))
        if step + AHEAD < SYSTEMS:
            for copy in load(step + AHEAD):
                copy.start()

    def lend(k):
        return pltpu.make_async_remote_copy(
            src_ref=lent.at[k], dst_ref=given.at[k], send_sem=lent_sem.at[k],
            recv_sem=given_sem.at[k], **device(me_row, 2 * x + 1 - core),
        )

    def scatter(k):
        hop = HOPS[k]
        target = 2 * xs[hop] + core
        for j in range(PLANE):
            if hop or j:
                pltpu.make_async_remote_copy(
                    src_ref=sums.at[k, row_at[j]], dst_ref=arrived.at[PLANE * LANDING[hop] + j],
                    send_sem=send_sem, recv_sem=recv_sem, **device(row_at[j], target),
                ).start()

        def diagonal():
            pltpu.make_async_remote_copy(
                src_ref=sums.at[k, PLANE, pl.ds(0, 8)], dst_ref=diagonals.at[PLANE * LANDING[hop] + to_first],
                send_sem=diag_send, recv_sem=diag_recv, **device(0, target),
            ).start()

        if hop:
            diagonal()
        else:
            pl.when(me_row != 0)(diagonal)
            arrived[0] = sums[k, me_row]

            @pl.when(me_row == 0)
            def _():
                diagonals[0] = sums[k, PLANE, 0:8]

    halves = {3: pl.ds(0, PLANE // 2), 1: pl.ds(PLANE // 2, PLANE // 2 + 1)}

    def relay(hop):
        return pltpu.make_async_remote_copy(
            src_ref=sums.at[0, halves[hop]], dst_ref=relayed.at[halves[hop]],
            send_sem=relay_send.at[hop], recv_sem=relay_recv.at[hop],
            **device(me_row, 2 * xs[hop] + core),
        )

    def combine(k):
        hop = HOPS[k]
        lend(k).wait_recv()
        sums[k] = sums[k] + given[k]
        if hop == 2:
            relay(1).start()
            relay(3).start()
            return
        if hop:
            relay(hop).wait_recv()
            sums[k, halves[hop]] = sums[k, halves[hop]] + relayed[halves[hop]]
        scatter(k)

    for step, (k, own) in enumerate(ORDER):
        gram(step, (sums if own else lent).at[k])
        if step == 0:
            pl.semaphore_wait(barrier, SENDERS - 1 + 5)
        if own:
            combine(k)
        else:
            lend(k).start()

    fetch_chosen.wait()
    chosen = chosen_ref[pl.ds(me_group, 1), :]
    coeffs[...] = (lax.broadcasted_iota(jnp.int32, (COLS, KEPT), 0) == chosen).astype(F32).T

    others = arrived.at[pl.ds(1, SENDERS - 1)]
    landed(others, recv_sem)

    def add(i, total):
        return total + arrived[i]

    pieces[me_row] = lax.fori_loop(1, SENDERS, add, arrived[0], unroll=47)

    def share(j, part, send, recv):
        return pltpu.make_async_remote_copy(
            src_ref=part, dst_ref=part, send_sem=send, recv_sem=recv, **device(row_at[j], me_group)
        )

    for j in range(1, PLANE):
        share(j, pieces.at[me_row], share_send, share_recv).start()
    fifteen = pieces.at[pl.ds(0, PLANE - 1)]
    shared_diagonal = pieces.at[PLANE, pl.ds(0, 8)]

    @pl.when(me_row == 0)
    def _():
        landed(diagonals.at[pl.ds(1, SENDERS - 1)], diag_recv)
        pieces[PLANE, 0:8, :] = lax.fori_loop(
            1, SENDERS, lambda i, total: total + diagonals[i], diagonals[0], unroll=47
        )
        for j in range(1, PLANE):
            share(j, shared_diagonal, share_diag_send, share_diag_recv).start()

    @pl.when(me_row != 0)
    def _():
        landed(shared_diagonal, share_diag_recv)

    landed(fifteen, share_recv)

    sub = lax.broadcasted_iota(jnp.int32, (8, 128), 0)
    mixed = stacked([pieces[i, 8:16, :] for i in range(PLANE)])
    mixed_t = mixed.T
    diagonal = jnp.broadcast_to(pieces[PLANE, 0:1, :], (COLS, COLS))
    gram_f = jnp.where(down < across, mixed, jnp.where(down == across, diagonal, mixed_t))
    gram_s = jnp.where(down >= across, mixed, mixed_t)
    by_row, by_col = unit_scale(gram_f)
    cross_t = stacked([pieces[i, 0:8, :] for i in range(PLANE)])
    step_matrix = solved(gram_f * by_row * by_col, cross_t * by_row, sub) * by_row
    moves = stacked([step_matrix, dot(gram_s, step_matrix, 1, 0)])

    def iterate(i, _):
        moved = dot(coeffs[...], moves, 1, 1)
        solution_t, weighted = moved[:, :COLS], moved[:, COLS:]
        metric = dot(solution_t, weighted, 1, 1) * (1.0 / total_rows)
        by_row, by_col = unit_scale(metric)
        metric = metric * by_row * by_col
        wide = jnp.concatenate([metric, jnp.zeros((KEPT, COLS - KEPT), F32)], axis=1)
        coeffs[...] = stacked(normalised_rows(tiles(wide), tiles(solution_t * by_row), sub))
        return 0

    lax.fori_loop(0, ITERS, iterate, 0)
    local_coeffs[...] = coeffs[...].astype(BF16)
    out_ref[me_group] = local_coeffs[...]
    both[...] = jnp.zeros_like(both)

    def tell(hop, same):
        target = 2 * xs[hop] + (core if same else 1 - core)
        return pltpu.make_async_remote_copy(
            src_ref=local_coeffs, dst_ref=out_ref.at[me_group], send_sem=done_send,
            recv_sem=done_recv.at[2 * hop + same], **device(me_row, target),
        )

    for hop, same in ((2, 1), (2, 0), (1, 1), (1, 0), (3, 1), (3, 0), (0, 0)):
        tell(hop, same).start()
    for i, step in enumerate(ROTATION_ORDER):
        k, same = ORDER[step]
        hop = HOPS[k]
        s = system_at(step, x, core)
        if i:
            landed(out_ref.at[s], done_recv.at[2 * ((4 - hop) % 4) + same])
        if i < TURNED:
            rotate(both.at[i % 2], out_ref[s], wq.at[step], turned.at[i])
    landed(out_ref.at[pl.ds(0, SYSTEMS - 1)], done_send)
    landed(fifteen, share_send)
    landed(others, send_sem)
    landed(diagonals.at[pl.ds(0, 2)], diag_send)

    @pl.when(me_row != 0)
    def _():
        landed(shared_diagonal, diag_send)

    @pl.when(me_row == 0)
    def _():
        landed(diagonals.at[pl.ds(0, PLANE - 1)], share_diag_send)

    for k in range(4):
        lend(k).wait_send()
    relay(1).wait_send()
    relay(3).wait_send()


def in_hbm(a):
    return pltpu.with_memory_space_constraint(a, pltpu.HBM)


def gathered(basis, image, selection, total_rows):
    piece = (16, COLS)
    dma = pltpu.SemaphoreType.DMA
    return pl.pallas_call(
        functools.partial(gather_kernel, total_rows),
        out_shape=[
            pltpu.VMEM((SYSTEMS, KEPT, COLS), BF16),
            pltpu.VMEM((SYSTEMS, DEPTH, 2 * COLS), BF16),
            pltpu.VMEM((TURNED, DEPTH, COLS), BF16),
        ],
        in_specs=[pl.BlockSpec(memory_space=pltpu.HBM)] * 3,
        out_specs=[pl.BlockSpec(memory_space=pltpu.VMEM)] * 3,
        scratch_shapes=[
            pltpu.VMEM((2, 2 * KEPT, 2 * COLS), BF16),
            pltpu.VMEM((SYSTEMS, KEPT), jnp.int32),
            pltpu.VMEM((4, PLANE + 1, *piece), F32),
            pltpu.VMEM((4, PLANE + 1, *piece), F32),
            pltpu.VMEM((4, PLANE + 1, *piece), F32),
            pltpu.VMEM((PLANE + 1, *piece), F32),
            pltpu.VMEM((SENDERS, *piece), F32),
            pltpu.VMEM((SENDERS, 8, COLS), F32),
            pltpu.VMEM((PLANE + 1, *piece), F32),
            pltpu.VMEM((KEPT, COLS), F32),
            pltpu.VMEM((KEPT, COLS), BF16),
            dma((SYSTEMS, 2)),
            dma((4,)),
            dma((4,)),
            dma((4,)),
            dma((4,)),
            *[dma] * 9,
            dma((SYSTEMS,)),
            dma,
        ],
        compiler_params=pltpu.CompilerParams(
            collective_id=0, has_side_effects=True, vmem_limit_bytes=16 * 2**20
        ),
        name="gather_solve",
    )(in_hbm(basis), in_hbm(image), in_hbm(selection))


def rotate_kernel(wq, turned, c_ref, o_hbm, both, out, sem):
    group = lax.axis_index("groups")
    x, core = group // 2, lax.rem(group, 2)

    def store(i):
        source = turned.at[i] if i < TURNED else out.at[i - TURNED]
        return pltpu.make_async_copy(
            source, o_hbm.at[system_at(ROTATION_ORDER[i], x, core)], sem.at[i]
        )

    for i in range(TURNED):
        store(i).start()
    both[...] = jnp.zeros_like(both)
    for i in range(TURNED, SYSTEMS):
        step = ROTATION_ORDER[i]
        coeffs = c_ref[system_at(step, x, core)]
        rotate(both.at[i % 2], coeffs, wq.at[step], out.at[i - TURNED])
        store(i).start()
    for i in range(SYSTEMS):
        store(i).wait()


def rotated(coeffs, wq, turned):
    return pl.pallas_call(
        rotate_kernel,
        out_shape=jax.ShapeDtypeStruct((SYSTEMS, DEPTH, COLS), BF16),
        in_specs=[pl.BlockSpec(memory_space=pltpu.VMEM)] * 3,
        out_specs=pl.BlockSpec(memory_space=pltpu.HBM),
        scratch_shapes=[
            pltpu.VMEM((2, 2 * KEPT, 2 * COLS), BF16),
            pltpu.VMEM((SYSTEMS - TURNED, DEPTH, COLS), BF16),
            pltpu.SemaphoreType.DMA((SYSTEMS,)),
        ],
        compiler_params=pltpu.CompilerParams(vmem_limit_bytes=16 * 2**20),
        name="rotate",
    )(wq, turned, coeffs)


def on_device(basis, image, selection):
    total_rows = basis.shape[1] * lax.axis_size("rows") * lax.axis_size("groups")
    return rotated(*gathered(basis, image, selection, total_rows))


def solution(mesh):
    in_specs = (P(None, ("rows", "groups"), None), P(None, ("rows", "groups"), None), P())
    out_specs = P(None, ("rows", "groups"), None)
    return jax.shard_map(
        on_device, mesh=mesh, in_specs=in_specs, out_specs=out_specs, check_vma=False
    )
```

```python
import functools

import jax
import jax.numpy as jnp
from jax import lax
from jax.experimental import pallas as pl
from jax.experimental.pallas import tpu as pltpu
from jax.sharding import PartitionSpec as P

ITERS = 3
TURNED = 4
F32 = jnp.float32
BF16 = jnp.bfloat16
SYSTEMS = 8
DEPTH = 4096
COLS = 128
KEPT = 64
PLANE = 16


def split(a):
    high = a.astype(BF16)
    rest = a - high.astype(F32)
    middle = rest.astype(BF16)
    return high, middle, (rest - middle.astype(F32)).astype(BF16)


def dot(a, b, over_a, over_b):
    dims = (((over_a,), (over_b,)), ((), ()))

    def both(p, q, r, s):
        return lax.dot_general(
            jnp.concatenate([p, q], axis=over_a), jnp.concatenate([r, s], axis=over_b), dims,
            preferred_element_type=F32,
        )

    (a1, a2, a3), (b1, b2, b3) = split(a), split(b)
    return both(a1, a2, b1, b1) + (both(a1, a2, b2, b2) + both(a1, a3, b3, b1))


def lane(tile, j):
    return jnp.broadcast_to(tile[:, j : j + 1], (8, 128))


def row(tile, j):
    return jnp.broadcast_to(tile[j : j + 1, :], (8, 128))


def added(parts):
    while len(parts) > 1:
        parts = [parts[i] + parts[i + 1] for i in range(0, len(parts), 2)]
    return parts[0]


def times(cols, tile):
    return added([cols[j] * row(tile, j) for j in range(8)])


def less(tile, cols, rows):
    return tile - added([cols[j] * rows[j] for j in range(8)])


def pivot_pair(v, j, sub):
    at, at_next = sub == j, sub == j + 1
    a, b1, b2, c = row(v[j], j), row(v[j + 1], j), row(v[j], j + 1), row(v[j + 1], j + 1)
    r = 1.0 / (a * c - b1 * b2)
    p = jnp.where(at, -1.0, jnp.where(at_next, 0.0, v[j]))
    q = jnp.where(at_next, -1.0, jnp.where(at, 0.0, v[j + 1]))
    v[j], v[j + 1] = r * (q * b2 - p * c), r * (p * b1 - q * a)
    for other in range(8):
        if other not in (j, j + 1):
            u, t = row(v[other], j), row(v[other], j + 1)
            moved = p * (c * u - b1 * t) + q * (a * t - b2 * u)
            v[other] = jnp.where(at | at_next, 0.0, v[other]) - r * moved
    return a, b1, b2, c, r


def stacked(parts):
    return jnp.concatenate(parts, axis=0)


def tiles(a):
    return [a[8 * i : 8 * i + 8] for i in range(a.shape[0] // 8)]


def gauss_jordan(f, x, start, sub):
    for k in range(8):
        v = [lane(f[k], start + 8 * k + j) + 0.0 for j in range(8)]
        cols = {
            i: [lane(f[i], start + 8 * k + j) for j in range(8)]
            for i in [*range(k + 1, 8), *range(k)]
        }
        for j in range(0, 8, 2):
            pivot_pair(v, j, sub)
        fk, xk = times(v, f[k]), times(v, x[k])
        fr = [row(fk, j) for j in range(8)]
        xr = [row(xk, j) for j in range(8)]
        for i in cols:
            f[i] = less(f[i], cols[i], fr)
            x[i] = less(x[i], cols[i], xr)
        f[k], x[k] = fk, xk


def solved(f, x, sub):
    half = f.shape[0] // 2
    left = lax.broadcasted_iota(jnp.int32, (half, 128), 1) < half
    zero = jnp.zeros((half, 128), F32)
    low = f[half:]
    ft, xt = tiles(f[:half]), tiles(x[:half])
    gauss_jordan(ft, xt, 0, sub)
    ft, xt = stacked(ft), stacked(xt)
    right = jnp.concatenate([stacked([ft, zero]), stacked([xt, zero])], axis=1)
    step = dot(jnp.where(left, low, 0.0), right, 1, 0)
    fl, xl = tiles(low - step[:, :128]), tiles(x[half:] - step[:, 128:])
    gauss_jordan(fl, xl, half, sub)
    xl = stacked(xl)
    return stacked([xt - dot(jnp.where(left, 0.0, ft), stacked([zero, xl]), 1, 0), xl])


def next_block(inverse, raw, below):
    g = [added([below[m] * row(inverse[j], m) for m in range(8)]) for j in range(8)]
    return [raw[i] - added([g[j] * row(below[j], i) for j in range(8)]) for i in range(8)]


def normalised_rows(m, y, sub):
    n = len(m)
    out = []
    v = [lane(m[0], j) + 0.0 for j in range(8)]
    for k in range(n):
        if k < n - 1:
            raw = [lane(m[k + 1], 8 * k + 8 + j) + 0.0 for j in range(8)]
        cols = {i: [lane(m[i], 8 * k + j) for j in range(8)] for i in range(k + 1, n)}
        if k < n - 1:
            cols[k + 1] = [c + 0.0 for c in cols[k + 1]]
        mine = y[k]
        scale = jnp.zeros((8, 128), F32)
        for j in range(0, 8, 2):
            p, q = v[j], v[j + 1]
            a, b1, b2, c, r = pivot_pair(v, j, sub)
            inverse_a = 1.0 / a
            g, h = row(mine, j), row(mine, j + 1)
            below = r * (p * (c * g - b1 * h) + q * (a * h - b2 * g))
            mine = mine - jnp.where(
                sub > j + 1, below, jnp.where(sub == j + 1, (b2 * inverse_a) * g, 0.0)
            )
            second = (a * c - b1 * b2) * inverse_a
            scale = jnp.where(sub == j, a, jnp.where(sub == j + 1, second, scale))
        out.append(mine * lax.rsqrt(scale))
        if k < n - 1:
            inverse = v
            v = next_block(inverse, raw, cols[k + 1])
            mk, yk = times(inverse, m[k]), times(inverse, y[k])
            mr = [row(mk, j) for j in range(8)]
            yr = [row(yk, j) for j in range(8)]
            for i in cols:
                m[i] = less(m[i], cols[i], mr)
                y[i] = less(y[i], cols[i], yr)
    return out


def unit_scale(m):
    on = lax.broadcasted_iota(jnp.int32, m.shape, 0) == lax.broadcasted_iota(jnp.int32, m.shape, 1)
    diagonal = jnp.where(on, m, 0.0)
    return [lax.rsqrt(jnp.sum(diagonal, axis=axis, keepdims=True)) for axis in (1, 0)]


HOPS = (2, 0, 1, 3)
ORDER = ((0, 0), (1, 0), (0, 1), (2, 0), (1, 1), (3, 0), (2, 1), (3, 1))
AHEAD = 4
LANDING = {0: 0, 1: 1, 3: 2}
SENDERS = 3 * PLANE


def system_at(step, x, core):
    k, own = ORDER[step]
    return 2 * lax.rem(x + HOPS[k], 4) + (core if own else 1 - core)


ROTATION_ORDER = tuple(ORDER.index(c) for c in ((1, 1), (1, 0), (2, 1), (2, 0), (3, 1), (3, 0), (0, 1), (0, 0)))


def rotate(both, coeffs, data, out):
    part = 512
    both[:KEPT, :COLS] = coeffs
    both[KEPT:, COLS:] = coeffs
    for at in range(0, DEPTH, part):
        out[at : at + part] = lax.dot_general(
            data[at : at + part], both[...], (((1,), (1,)), ((), ())), preferred_element_type=F32
        ).astype(BF16)


def gather_kernel(
    total_rows, w_hbm, q_hbm, chosen_hbm, out_ref, wq, turned,
    both, chosen_ref, lent, given, sums, relayed, arrived, diagonals, pieces, coeffs, local_coeffs,
    load_sem, lent_sem, given_sem, relay_send, relay_recv, send_sem, recv_sem, diag_send, diag_recv,
    share_send, share_recv, share_diag_send, share_diag_recv, done_send, done_recv, chosen_sem,
):
    me_row, me_group = lax.axis_index("rows"), lax.axis_index("groups")
    x, core = me_group // 2, lax.rem(me_group, 2)
    y, z = me_row // 4, lax.rem(me_row, 4)
    xs, ys, zs = ([lax.rem(c + d, 4) for d in range(4)] for c in (x, y, z))
    row_at = [4 * ys[j // 4] + zs[j % 4] for j in range(PLANE)]
    to_first = 4 * lax.rem(4 - y, 4) + lax.rem(4 - z, 4)

    def device(rows, groups):
        return dict(
            device_id={"rows": rows, "groups": groups}, device_id_type=pl.DeviceIdType.MESH
        )

    def landed(ref, sem):
        pltpu.make_async_copy(ref, ref, sem).wait()

    def load(step):
        s = system_at(step, x, core)
        return [
            pltpu.make_async_copy(ref.at[s], wq.at[step, :, pl.ds(off, COLS)], load_sem.at[step, i])
            for i, (ref, off) in enumerate(((w_hbm, 0), (q_hbm, COLS)))
        ]

    for step in range(AHEAD):
        for copy in load(step):
            copy.start()
    fetch_chosen = pltpu.make_async_copy(chosen_hbm, chosen_ref, chosen_sem)
    fetch_chosen.start()

    barrier = pltpu.get_barrier_semaphore()
    for hop in range(4):
        pl.semaphore_signal(barrier, inc=1, **device(me_row, 2 * xs[hop] + 1 - core))
        for j in range(PLANE if hop != 2 else 1):
            if hop or j:
                pl.semaphore_signal(barrier, inc=1, **device(row_at[j], 2 * xs[hop] + core))

    across = lax.broadcasted_iota(jnp.int32, (COLS, COLS), 1)
    down = lax.broadcasted_iota(jnp.int32, (COLS, COLS), 0)

    def gram(step, ref):
        for copy in load(step):
            copy.wait()
        if step + AHEAD < SYSTEMS:
            for copy in load(step + AHEAD):
                copy.start()
        over_rows = (((0,), (0,)), ((), ()))
        w, q = wq[step, :, :COLS], wq[step, :, COLS:]
        gram_s = lax.dot_general(w, w, over_rows, preferred_element_type=F32)
        g = lax.dot_general(q, wq[step], over_rows, preferred_element_type=F32)
        gram_f = g[:, COLS:]
        ref[pl.ds(0, PLANE), 0:8, :] = g[:, :COLS].reshape(PLANE, 8, COLS)
        ref[pl.ds(0, PLANE), 8:16, :] = jnp.where(down >= across, gram_s, gram_f).reshape(
            PLANE, 8, COLS
        )
        diagonal = jnp.sum(jnp.where(down == across, gram_f, 0.0), axis=0, keepdims=True)
        ref[PLANE] = jnp.broadcast_to(diagonal, (16, COLS))

    def lend(k):
        return pltpu.make_async_remote_copy(
            src_ref=lent.at[k], dst_ref=given.at[k], send_sem=lent_sem.at[k],
            recv_sem=given_sem.at[k], **device(me_row, 2 * x + 1 - core),
        )

    def scatter(k):
        hop = HOPS[k]
        target = 2 * xs[hop] + core
        for j in range(PLANE):
            if hop or j:
                pltpu.make_async_remote_copy(
                    src_ref=sums.at[k, row_at[j]], dst_ref=arrived.at[PLANE * LANDING[hop] + j],
                    send_sem=send_sem, recv_sem=recv_sem, **device(row_at[j], target),
                ).start()

        def diagonal():
            pltpu.make_async_remote_copy(
                src_ref=sums.at[k, PLANE, pl.ds(0, 8)], dst_ref=diagonals.at[PLANE * LANDING[hop] + to_first],
                send_sem=diag_send, recv_sem=diag_recv, **device(0, target),
            ).start()

        if hop:
            diagonal()
        else:
            pl.when(me_row != 0)(diagonal)
            arrived[0] = sums[k, me_row]

            @pl.when(me_row == 0)
            def _():
                diagonals[0] = sums[k, PLANE, 0:8]

    halves = {3: pl.ds(0, PLANE // 2), 1: pl.ds(PLANE // 2, PLANE // 2 + 1)}

    def relay(hop):
        return pltpu.make_async_remote_copy(
            src_ref=sums.at[0, halves[hop]], dst_ref=relayed.at[halves[hop]],
            send_sem=relay_send.at[hop], recv_sem=relay_recv.at[hop],
            **device(me_row, 2 * xs[hop] + core),
        )

    def combine(k):
        hop = HOPS[k]
        lend(k).wait_recv()
        sums[k] = sums[k] + given[k]
        if hop == 2:
            relay(1).start()
            relay(3).start()
            return
        if hop:
            relay(hop).wait_recv()
            sums[k, halves[hop]] = sums[k, halves[hop]] + relayed[halves[hop]]
        scatter(k)

    for step, (k, own) in enumerate(ORDER):
        gram(step, (sums if own else lent).at[k])
        if step == 0:
            pl.semaphore_wait(barrier, SENDERS - 1 + 5)
        if own:
            combine(k)
        else:
            lend(k).start()

    fetch_chosen.wait()
    chosen = chosen_ref[pl.ds(me_group, 1), :]
    coeffs[...] = (lax.broadcasted_iota(jnp.int32, (COLS, KEPT), 0) == chosen).astype(F32).T

    others = arrived.at[pl.ds(1, SENDERS - 1)]
    landed(others, recv_sem)

    def add(i, total):
        return total + arrived[i]

    pieces[me_row] = lax.fori_loop(1, SENDERS, add, arrived[0], unroll=47)

    def share(j, part, send, recv):
        return pltpu.make_async_remote_copy(
            src_ref=part, dst_ref=part, send_sem=send, recv_sem=recv, **device(row_at[j], me_group)
        )

    for j in range(1, PLANE):
        share(j, pieces.at[me_row], share_send, share_recv).start()
    fifteen = pieces.at[pl.ds(0, PLANE - 1)]
    shared_diagonal = pieces.at[PLANE, pl.ds(0, 8)]

    @pl.when(me_row == 0)
    def _():
        landed(diagonals.at[pl.ds(1, SENDERS - 1)], diag_recv)
        pieces[PLANE, 0:8, :] = lax.fori_loop(
            1, SENDERS, lambda i, total: total + diagonals[i], diagonals[0], unroll=47
        )
        for j in range(1, PLANE):
            share(j, shared_diagonal, share_diag_send, share_diag_recv).start()

    @pl.when(me_row != 0)
    def _():
        landed(shared_diagonal, share_diag_recv)

    landed(fifteen, share_recv)

    sub = lax.broadcasted_iota(jnp.int32, (8, 128), 0)
    mixed = stacked([pieces[i, 8:16, :] for i in range(PLANE)])
    mixed_t = mixed.T
    diagonal = jnp.broadcast_to(pieces[PLANE, 0:1, :], (COLS, COLS))
    gram_f = jnp.where(down < across, mixed, jnp.where(down == across, diagonal, mixed_t))
    gram_s = jnp.where(down >= across, mixed, mixed_t)
    by_row, by_col = unit_scale(diagonal)
    cross_t = stacked([pieces[i, 0:8, :] for i in range(PLANE)])
    step_matrix = solved(gram_f * by_row * by_col, cross_t * by_row, sub) * by_row
    moves = stacked([step_matrix, dot(gram_s, step_matrix, 1, 0)])

    def iterate(i, _):
        moved = dot(coeffs[...], moves, 1, 1)
        solution_t, weighted = moved[:, :COLS], moved[:, COLS:]
        metric = dot(solution_t, weighted, 1, 1) * (1.0 / total_rows)
        by_row, by_col = unit_scale(metric)
        metric = metric * by_row * by_col
        wide = jnp.concatenate([metric, jnp.zeros((KEPT, COLS - KEPT), F32)], axis=1)
        coeffs[...] = stacked(normalised_rows(tiles(wide), tiles(solution_t * by_row), sub))
        return 0

    lax.fori_loop(0, ITERS, iterate, 0)
    local_coeffs[...] = coeffs[...].astype(BF16)
    out_ref[me_group] = local_coeffs[...]
    both[...] = jnp.zeros_like(both)

    def tell(hop, same):
        target = 2 * xs[hop] + (core if same else 1 - core)
        return pltpu.make_async_remote_copy(
            src_ref=local_coeffs, dst_ref=out_ref.at[me_group], send_sem=done_send,
            recv_sem=done_recv.at[2 * hop + same], **device(me_row, target),
        )

    for hop, same in ((2, 1), (2, 0), (1, 1), (1, 0), (3, 1), (3, 0), (0, 0)):
        tell(hop, same).start()
    for i, step in enumerate(ROTATION_ORDER):
        k, same = ORDER[step]
        hop = HOPS[k]
        s = system_at(step, x, core)
        if i:
            landed(out_ref.at[s], done_recv.at[2 * ((4 - hop) % 4) + same])
        if i < TURNED:
            rotate(both.at[i % 2], out_ref[s], wq.at[step], turned.at[i])
    landed(out_ref.at[pl.ds(0, SYSTEMS - 1)], done_send)
    landed(fifteen, share_send)
    landed(others, send_sem)
    landed(diagonals.at[pl.ds(0, 2)], diag_send)

    @pl.when(me_row != 0)
    def _():
        landed(shared_diagonal, diag_send)

    @pl.when(me_row == 0)
    def _():
        landed(diagonals.at[pl.ds(0, PLANE - 1)], share_diag_send)

    for k in range(4):
        lend(k).wait_send()
    relay(1).wait_send()
    relay(3).wait_send()


def in_hbm(a):
    return pltpu.with_memory_space_constraint(a, pltpu.HBM)


def gathered(basis, image, selection, total_rows):
    piece = (16, COLS)
    dma = pltpu.SemaphoreType.DMA
    return pl.pallas_call(
        functools.partial(gather_kernel, total_rows),
        out_shape=[
            pltpu.VMEM((SYSTEMS, KEPT, COLS), BF16),
            pltpu.VMEM((SYSTEMS, DEPTH, 2 * COLS), BF16),
            pltpu.VMEM((TURNED, DEPTH, COLS), BF16),
        ],
        in_specs=[pl.BlockSpec(memory_space=pltpu.HBM)] * 3,
        out_specs=[pl.BlockSpec(memory_space=pltpu.VMEM)] * 3,
        scratch_shapes=[
            pltpu.VMEM((2, 2 * KEPT, 2 * COLS), BF16),
            pltpu.VMEM((SYSTEMS, KEPT), jnp.int32),
            pltpu.VMEM((4, PLANE + 1, *piece), F32),
            pltpu.VMEM((4, PLANE + 1, *piece), F32),
            pltpu.VMEM((4, PLANE + 1, *piece), F32),
            pltpu.VMEM((PLANE + 1, *piece), F32),
            pltpu.VMEM((SENDERS, *piece), F32),
            pltpu.VMEM((SENDERS, 8, COLS), F32),
            pltpu.VMEM((PLANE + 1, *piece), F32),
            pltpu.VMEM((KEPT, COLS), F32),
            pltpu.VMEM((KEPT, COLS), BF16),
            dma((SYSTEMS, 2)),
            dma((4,)),
            dma((4,)),
            dma((4,)),
            dma((4,)),
            *[dma] * 9,
            dma((SYSTEMS,)),
            dma,
        ],
        compiler_params=pltpu.CompilerParams(
            collective_id=0, has_side_effects=True, vmem_limit_bytes=16 * 2**20
        ),
        name="gather_solve",
    )(in_hbm(basis), in_hbm(image), in_hbm(selection))


def rotate_kernel(wq, turned, c_ref, o_hbm, both, out, sem):
    group = lax.axis_index("groups")
    x, core = group // 2, lax.rem(group, 2)

    def store(i):
        source = turned.at[i] if i < TURNED else out.at[i - TURNED]
        return pltpu.make_async_copy(
            source, o_hbm.at[system_at(ROTATION_ORDER[i], x, core)], sem.at[i]
        )

    for i in range(TURNED):
        store(i).start()
    both[...] = jnp.zeros_like(both)
    for i in range(TURNED, SYSTEMS):
        step = ROTATION_ORDER[i]
        coeffs = c_ref[system_at(step, x, core)]
        rotate(both.at[i % 2], coeffs, wq.at[step], out.at[i - TURNED])
        store(i).start()
    for i in range(SYSTEMS):
        store(i).wait()


def rotated(coeffs, wq, turned):
    return pl.pallas_call(
        rotate_kernel,
        out_shape=jax.ShapeDtypeStruct((SYSTEMS, DEPTH, COLS), BF16),
        in_specs=[pl.BlockSpec(memory_space=pltpu.VMEM)] * 3,
        out_specs=pl.BlockSpec(memory_space=pltpu.HBM),
        scratch_shapes=[
            pltpu.VMEM((2, 2 * KEPT, 2 * COLS), BF16),
            pltpu.VMEM((SYSTEMS - TURNED, DEPTH, COLS), BF16),
            pltpu.SemaphoreType.DMA((SYSTEMS,)),
        ],
        compiler_params=pltpu.CompilerParams(vmem_limit_bytes=16 * 2**20),
        name="rotate",
    )(wq, turned, coeffs)


def on_device(basis, image, selection):
    total_rows = basis.shape[1] * lax.axis_size("rows") * lax.axis_size("groups")
    return rotated(*gathered(basis, image, selection, total_rows))


def solution(mesh):
    in_specs = (P(None, ("rows", "groups"), None), P(None, ("rows", "groups"), None), P())
    out_specs = P(None, ("rows", "groups"), None)
    return jax.shard_map(
        on_device, mesh=mesh, in_specs=in_specs, out_specs=out_specs, check_vma=False
    )
```

```python
import functools

import jax
import jax.numpy as jnp
from jax import lax
from jax.experimental import pallas as pl
from jax.experimental.pallas import tpu as pltpu
from jax.sharding import PartitionSpec as P

ITERS = 3
TURNED = 4
F32 = jnp.float32
BF16 = jnp.bfloat16
SYSTEMS = 8
DEPTH = 4096
COLS = 128
KEPT = 64
PLANE = 16


def split(a):
    high = a.astype(BF16)
    rest = a - high.astype(F32)
    middle = rest.astype(BF16)
    return high, middle, (rest - middle.astype(F32)).astype(BF16)


def right_parts(b, over_b):
    b1, b2, b3 = split(b)
    return [jnp.concatenate(pair, axis=over_b) for pair in ((b1, b1), (b2, b2), (b3, b1))]


def dot(a, b, over_a, over_b, parts=None):
    dims = (((over_a,), (over_b,)), ((), ()))
    a1, a2, a3 = split(a)
    a12, a13 = (jnp.concatenate([a1, other], axis=over_a) for other in (a2, a3))
    terms = [
        lax.dot_general(left, right, dims, preferred_element_type=F32)
        for left, right in zip((a12, a12, a13), parts or right_parts(b, over_b))
    ]
    return terms[0] + (terms[1] + terms[2])


def lane(tile, j):
    return jnp.broadcast_to(tile[:, j : j + 1], (8, 128))


def row(tile, j):
    return jnp.broadcast_to(tile[j : j + 1, :], (8, 128))


def added(parts):
    while len(parts) > 1:
        parts = [parts[i] + parts[i + 1] for i in range(0, len(parts), 2)]
    return parts[0]


def times(cols, tile):
    return added([cols[j] * row(tile, j) for j in range(8)])


def less(tile, cols, rows):
    return tile - added([cols[j] * rows[j] for j in range(8)])


def pivot_pair(v, j, sub):
    at, at_next = sub == j, sub == j + 1
    a, b1, b2, c = row(v[j], j), row(v[j + 1], j), row(v[j], j + 1), row(v[j + 1], j + 1)
    r = 1.0 / (a * c - b1 * b2)
    p = jnp.where(at, -1.0, jnp.where(at_next, 0.0, v[j]))
    q = jnp.where(at_next, -1.0, jnp.where(at, 0.0, v[j + 1]))
    v[j], v[j + 1] = r * (q * b2 - p * c), r * (p * b1 - q * a)
    for other in range(8):
        if other not in (j, j + 1):
            u, t = row(v[other], j), row(v[other], j + 1)
            moved = p * (c * u - b1 * t) + q * (a * t - b2 * u)
            v[other] = jnp.where(at | at_next, 0.0, v[other]) - r * moved
    return a, b1, b2, c, r


def stacked(parts):
    return jnp.concatenate(parts, axis=0)


def tiles(a):
    return [a[8 * i : 8 * i + 8] for i in range(a.shape[0] // 8)]


def gauss_jordan(f, x, start, sub):
    for k in range(8):
        v = [lane(f[k], start + 8 * k + j) + 0.0 for j in range(8)]
        cols = {
            i: [lane(f[i], start + 8 * k + j) for j in range(8)]
            for i in [*range(k + 1, 8), *range(k)]
        }
        for j in range(0, 8, 2):
            pivot_pair(v, j, sub)
        fk, xk = times(v, f[k]), times(v, x[k])
        fr = [row(fk, j) for j in range(8)]
        xr = [row(xk, j) for j in range(8)]
        for i in cols:
            f[i] = less(f[i], cols[i], fr)
            x[i] = less(x[i], cols[i], xr)
        f[k], x[k] = fk, xk


def solved(f, x, sub):
    half = f.shape[0] // 2
    left = lax.broadcasted_iota(jnp.int32, (half, 128), 1) < half
    zero = jnp.zeros((half, 128), F32)
    low = f[half:]
    ft, xt = tiles(f[:half]), tiles(x[:half])
    gauss_jordan(ft, xt, 0, sub)
    ft, xt = stacked(ft), stacked(xt)
    right = jnp.concatenate([stacked([ft, zero]), stacked([xt, zero])], axis=1)
    step = dot(jnp.where(left, low, 0.0), right, 1, 0)
    fl, xl = tiles(low - step[:, :128]), tiles(x[half:] - step[:, 128:])
    gauss_jordan(fl, xl, half, sub)
    xl = stacked(xl)
    return stacked([xt - dot(jnp.where(left, 0.0, ft), stacked([zero, xl]), 1, 0), xl])


def next_block(inverse, raw, below):
    g = [added([below[m] * row(inverse[j], m) for m in range(8)]) for j in range(8)]
    return [raw[i] - added([g[j] * row(below[j], i) for j in range(8)]) for i in range(8)]


def normalised_rows(m, y, sub):
    n = len(m)
    out = []
    v = [lane(m[0], j) + 0.0 for j in range(8)]
    for k in range(n):
        if k < n - 1:
            raw = [lane(m[k + 1], 8 * k + 8 + j) + 0.0 for j in range(8)]
        cols = {i: [lane(m[i], 8 * k + j) for j in range(8)] for i in range(k + 1, n)}
        if k < n - 1:
            cols[k + 1] = [c + 0.0 for c in cols[k + 1]]
        mine = y[k]
        scale = jnp.zeros((8, 128), F32)
        for j in range(0, 8, 2):
            p, q = v[j], v[j + 1]
            a, b1, b2, c, r = pivot_pair(v, j, sub)
            inverse_a = 1.0 / a
            g, h = row(mine, j), row(mine, j + 1)
            below = r * (p * (c * g - b1 * h) + q * (a * h - b2 * g))
            mine = mine - jnp.where(
                sub > j + 1, below, jnp.where(sub == j + 1, (b2 * inverse_a) * g, 0.0)
            )
            second = (a * c - b1 * b2) * inverse_a
            scale = jnp.where(sub == j, a, jnp.where(sub == j + 1, second, scale))
        out.append(mine * lax.rsqrt(scale))
        if k < n - 1:
            inverse = v
            v = next_block(inverse, raw, cols[k + 1])
            mk, yk = times(inverse, m[k]), times(inverse, y[k])
            mr = [row(mk, j) for j in range(8)]
            yr = [row(yk, j) for j in range(8)]
            for i in cols:
                m[i] = less(m[i], cols[i], mr)
                y[i] = less(y[i], cols[i], yr)
    return out


def unit_scale(m):
    on = lax.broadcasted_iota(jnp.int32, m.shape, 0) == lax.broadcasted_iota(jnp.int32, m.shape, 1)
    diagonal = jnp.where(on, m, 0.0)
    return [lax.rsqrt(jnp.sum(diagonal, axis=axis, keepdims=True)) for axis in (1, 0)]


HOPS = (2, 0, 1, 3)
ORDER = ((0, 0), (1, 0), (0, 1), (2, 0), (1, 1), (3, 0), (2, 1), (3, 1))
AHEAD = 4
FAR_FIRST = sorted(range(PLANE), key=lambda j: -sum((0, 1, 2, 1)[c] for c in (j // 4, j % 4)))
LANDING = {0: 0, 1: 1, 3: 2}
SENDERS = 3 * PLANE


def system_at(step, x, core):
    k, own = ORDER[step]
    return 2 * lax.rem(x + HOPS[k], 4) + (core if own else 1 - core)


ROTATION_ORDER = tuple(ORDER.index(c) for c in ((1, 1), (1, 0), (2, 1), (2, 0), (3, 1), (3, 0), (0, 1), (0, 0)))


def rotate(both, coeffs, data, out):
    part = 512
    both[:KEPT, :COLS] = coeffs
    both[KEPT:, COLS:] = coeffs
    for at in range(0, DEPTH, part):
        out[at : at + part] = lax.dot_general(
            data[at : at + part], both[...], (((1,), (1,)), ((), ())), preferred_element_type=F32
        ).astype(BF16)


def gather_kernel(
    total_rows, w_hbm, q_hbm, chosen_hbm, out_ref, wq, turned,
    both, chosen_ref, lent, given, sums, relayed, arrived, diagonals, pieces, moves_ref, coeffs, local_coeffs,
    load_sem, lent_sem, given_sem, relay_send, relay_recv, send_sem, recv_sem, diag_send, diag_recv,
    share_send, share_recv, share_diag_send, share_diag_recv, done_send, done_recv, chosen_sem,
):
    me_row, me_group = lax.axis_index("rows"), lax.axis_index("groups")
    x, core = me_group // 2, lax.rem(me_group, 2)
    y, z = me_row // 4, lax.rem(me_row, 4)
    xs, ys, zs = ([lax.rem(c + d, 4) for d in range(4)] for c in (x, y, z))
    row_at = [4 * ys[j // 4] + zs[j % 4] for j in range(PLANE)]
    to_first = 4 * lax.rem(4 - y, 4) + lax.rem(4 - z, 4)

    def device(rows, groups):
        return dict(
            device_id={"rows": rows, "groups": groups}, device_id_type=pl.DeviceIdType.MESH
        )

    def landed(ref, sem):
        pltpu.make_async_copy(ref, ref, sem).wait()

    def load(step):
        s = system_at(step, x, core)
        return [
            pltpu.make_async_copy(ref.at[s], wq.at[step, :, pl.ds(off, COLS)], load_sem.at[step, i])
            for i, (ref, off) in enumerate(((w_hbm, 0), (q_hbm, COLS)))
        ]

    for step in range(AHEAD):
        for copy in load(step):
            copy.start()
    fetch_chosen = pltpu.make_async_copy(chosen_hbm, chosen_ref, chosen_sem)
    fetch_chosen.start()

    barrier = pltpu.get_barrier_semaphore()
    for hop in range(4):
        pl.semaphore_signal(barrier, inc=1, **device(me_row, 2 * xs[hop] + 1 - core))
        for j in range(PLANE if hop != 2 else 1):
            if hop or j:
                pl.semaphore_signal(barrier, inc=1, **device(row_at[j], 2 * xs[hop] + core))

    across = lax.broadcasted_iota(jnp.int32, (COLS, COLS), 1)
    down = lax.broadcasted_iota(jnp.int32, (COLS, COLS), 0)

    def gram(step, ref):
        for copy in load(step):
            copy.wait()
        if step + AHEAD < SYSTEMS:
            for copy in load(step + AHEAD):
                copy.start()
        over_rows = (((0,), (0,)), ((), ()))
        w, q = wq[step, :, :COLS], wq[step, :, COLS:]
        gram_s = lax.dot_general(w, w, over_rows, preferred_element_type=F32)
        g = lax.dot_general(q, wq[step], over_rows, preferred_element_type=F32)
        gram_f = g[:, COLS:]
        ref[pl.ds(0, PLANE), 0:8, :] = g[:, :COLS].reshape(PLANE, 8, COLS)
        ref[pl.ds(0, PLANE), 8:16, :] = jnp.where(down >= across, gram_s, gram_f).reshape(
            PLANE, 8, COLS
        )
        diagonal = jnp.sum(jnp.where(down == across, gram_f, 0.0), axis=0, keepdims=True)
        ref[PLANE] = jnp.broadcast_to(diagonal, (16, COLS))

    def lend(k):
        return pltpu.make_async_remote_copy(
            src_ref=lent.at[k], dst_ref=given.at[k], send_sem=lent_sem.at[k],
            recv_sem=given_sem.at[k], **device(me_row, 2 * x + 1 - core),
        )

    def scatter(k):
        hop = HOPS[k]
        target = 2 * xs[hop] + core

        def diagonal():
            pltpu.make_async_remote_copy(
                src_ref=sums.at[k, PLANE, pl.ds(0, 8)], dst_ref=diagonals.at[PLANE * LANDING[hop] + to_first],
                send_sem=diag_send, recv_sem=diag_recv, **device(0, target),
            ).start()

        if hop:
            diagonal()
        else:
            pl.when(me_row != 0)(diagonal)
            arrived[0] = sums[k, me_row]

            @pl.when(me_row == 0)
            def _():
                diagonals[0] = sums[k, PLANE, 0:8]

        for j in FAR_FIRST:
            if hop or j:
                pltpu.make_async_remote_copy(
                    src_ref=sums.at[k, row_at[j]], dst_ref=arrived.at[PLANE * LANDING[hop] + j],
                    send_sem=send_sem, recv_sem=recv_sem, **device(row_at[j], target),
                ).start()

    halves = {3: pl.ds(0, PLANE // 2), 1: pl.ds(PLANE // 2, PLANE // 2 + 1)}

    def relay(hop):
        return pltpu.make_async_remote_copy(
            src_ref=sums.at[0, halves[hop]], dst_ref=relayed.at[halves[hop]],
            send_sem=relay_send.at[hop], recv_sem=relay_recv.at[hop],
            **device(me_row, 2 * xs[hop] + core),
        )

    def combine(k):
        hop = HOPS[k]
        lend(k).wait_recv()
        sums[k] = sums[k] + given[k]
        if hop == 2:
            relay(1).start()
            relay(3).start()
            return
        if hop:
            relay(hop).wait_recv()
            sums[k, halves[hop]] = sums[k, halves[hop]] + relayed[halves[hop]]
        scatter(k)

    for step, (k, own) in enumerate(ORDER):
        gram(step, (sums if own else lent).at[k])
        if step == 0:
            pl.semaphore_wait(barrier, SENDERS - 1 + 5)
        if own:
            combine(k)
        else:
            lend(k).start()

    fetch_chosen.wait()
    chosen = chosen_ref[pl.ds(me_group, 1), :]
    coeffs[...] = (lax.broadcasted_iota(jnp.int32, (COLS, KEPT), 0) == chosen).astype(F32).T

    def share(j, part, send, recv):
        return pltpu.make_async_remote_copy(
            src_ref=part, dst_ref=part, send_sem=send, recv_sem=recv, **device(row_at[j], me_group)
        )

    shared_diagonal = pieces.at[PLANE, pl.ds(0, 8)]

    @pl.when(me_row == 0)
    def _():
        landed(diagonals.at[pl.ds(1, SENDERS - 1)], diag_recv)
        pieces[PLANE, 0:8, :] = lax.fori_loop(
            1, SENDERS, lambda i, total: total + diagonals[i], diagonals[0], unroll=47
        )
        for j in FAR_FIRST[:-1]:
            share(j, shared_diagonal, share_diag_send, share_diag_recv).start()

    others = arrived.at[pl.ds(1, SENDERS - 1)]
    landed(others, recv_sem)

    def add(i, total):
        return total + arrived[i]

    pieces[me_row] = lax.fori_loop(1, SENDERS, add, arrived[0], unroll=47)

    for j in FAR_FIRST[:-1]:
        share(j, pieces.at[me_row], share_send, share_recv).start()
    fifteen = pieces.at[pl.ds(0, PLANE - 1)]

    @pl.when(me_row != 0)
    def _():
        landed(shared_diagonal, share_diag_recv)

    landed(fifteen, share_recv)

    sub = lax.broadcasted_iota(jnp.int32, (8, 128), 0)
    mixed = stacked([pieces[i, 8:16, :] for i in range(PLANE)])
    mixed_t = mixed.T
    diagonal = jnp.broadcast_to(pieces[PLANE, 0:1, :], (COLS, COLS))
    gram_f = jnp.where(down < across, mixed, jnp.where(down == across, diagonal, mixed_t))
    gram_s = jnp.where(down >= across, mixed, mixed_t)
    by_row, by_col = unit_scale(diagonal)
    cross_t = stacked([pieces[i, 0:8, :] for i in range(PLANE)])
    step_matrix = solved(gram_f * by_row * by_col, cross_t * by_row, sub) * by_row
    moves = stacked([step_matrix, dot(gram_s, step_matrix, 1, 0)])

    for i, part in enumerate(right_parts(moves, 1)):
        moves_ref[i] = part

    def iterate(i, _):
        moved = dot(coeffs[...], None, 1, 1, [moves_ref[i] for i in range(3)])
        solution_t, weighted = moved[:, :COLS], moved[:, COLS:]
        metric = dot(solution_t, weighted, 1, 1) * (1.0 / total_rows)
        by_row, by_col = unit_scale(metric)
        metric = metric * by_row * by_col
        wide = jnp.concatenate([metric, jnp.zeros((KEPT, COLS - KEPT), F32)], axis=1)
        coeffs[...] = stacked(normalised_rows(tiles(wide), tiles(solution_t * by_row), sub))
        return 0

    lax.fori_loop(0, ITERS, iterate, 0)
    local_coeffs[...] = coeffs[...].astype(BF16)
    out_ref[me_group] = local_coeffs[...]
    both[...] = jnp.zeros_like(both)

    def tell(hop, same):
        target = 2 * xs[hop] + (core if same else 1 - core)
        return pltpu.make_async_remote_copy(
            src_ref=local_coeffs, dst_ref=out_ref.at[me_group], send_sem=done_send,
            recv_sem=done_recv.at[2 * hop + same], **device(me_row, target),
        )

    for hop, same in ((2, 1), (2, 0), (1, 1), (1, 0), (3, 1), (3, 0), (0, 0)):
        tell(hop, same).start()
    for i, step in enumerate(ROTATION_ORDER):
        k, same = ORDER[step]
        hop = HOPS[k]
        s = system_at(step, x, core)
        if i:
            landed(out_ref.at[s], done_recv.at[2 * ((4 - hop) % 4) + same])
        if i < TURNED:
            rotate(both.at[i % 2], out_ref[s], wq.at[step], turned.at[i])
    landed(out_ref.at[pl.ds(0, SYSTEMS - 1)], done_send)
    landed(fifteen, share_send)
    landed(others, send_sem)
    landed(diagonals.at[pl.ds(0, 2)], diag_send)

    @pl.when(me_row != 0)
    def _():
        landed(shared_diagonal, diag_send)

    @pl.when(me_row == 0)
    def _():
        landed(diagonals.at[pl.ds(0, PLANE - 1)], share_diag_send)

    for k in range(4):
        lend(k).wait_send()
    relay(1).wait_send()
    relay(3).wait_send()


def in_hbm(a):
    return pltpu.with_memory_space_constraint(a, pltpu.HBM)


def gathered(basis, image, selection, total_rows):
    piece = (16, COLS)
    dma = pltpu.SemaphoreType.DMA
    return pl.pallas_call(
        functools.partial(gather_kernel, total_rows),
        out_shape=[
            pltpu.VMEM((SYSTEMS, KEPT, COLS), BF16),
            pltpu.VMEM((SYSTEMS, DEPTH, 2 * COLS), BF16),
            pltpu.VMEM((TURNED, DEPTH, COLS), BF16),
        ],
        in_specs=[pl.BlockSpec(memory_space=pltpu.HBM)] * 3,
        out_specs=[pl.BlockSpec(memory_space=pltpu.VMEM)] * 3,
        scratch_shapes=[
            pltpu.VMEM((2, 2 * KEPT, 2 * COLS), BF16),
            pltpu.VMEM((SYSTEMS, KEPT), jnp.int32),
            pltpu.VMEM((4, PLANE + 1, *piece), F32),
            pltpu.VMEM((4, PLANE + 1, *piece), F32),
            pltpu.VMEM((4, PLANE + 1, *piece), F32),
            pltpu.VMEM((PLANE + 1, *piece), F32),
            pltpu.VMEM((SENDERS, *piece), F32),
            pltpu.VMEM((SENDERS, 8, COLS), F32),
            pltpu.VMEM((PLANE + 1, *piece), F32),
            pltpu.VMEM((3, 2 * COLS, 2 * COLS), BF16),
            pltpu.VMEM((KEPT, COLS), F32),
            pltpu.VMEM((KEPT, COLS), BF16),
            dma((SYSTEMS, 2)),
            dma((4,)),
            dma((4,)),
            dma((4,)),
            dma((4,)),
            *[dma] * 9,
            dma((SYSTEMS,)),
            dma,
        ],
        compiler_params=pltpu.CompilerParams(
            collective_id=0, has_side_effects=True, vmem_limit_bytes=16 * 2**20
        ),
        name="gather_solve",
    )(in_hbm(basis), in_hbm(image), in_hbm(selection))


def rotate_kernel(wq, turned, c_ref, o_hbm, both, out, sem):
    group = lax.axis_index("groups")
    x, core = group // 2, lax.rem(group, 2)

    def store(i):
        source = turned.at[i] if i < TURNED else out.at[i - TURNED]
        return pltpu.make_async_copy(
            source, o_hbm.at[system_at(ROTATION_ORDER[i], x, core)], sem.at[i]
        )

    for i in range(TURNED):
        store(i).start()
    both[...] = jnp.zeros_like(both)
    for i in range(TURNED, SYSTEMS):
        step = ROTATION_ORDER[i]
        coeffs = c_ref[system_at(step, x, core)]
        rotate(both.at[i % 2], coeffs, wq.at[step], out.at[i - TURNED])
        store(i).start()
    for i in range(SYSTEMS):
        store(i).wait()


def rotated(coeffs, wq, turned):
    return pl.pallas_call(
        rotate_kernel,
        out_shape=jax.ShapeDtypeStruct((SYSTEMS, DEPTH, COLS), BF16),
        in_specs=[pl.BlockSpec(memory_space=pltpu.VMEM)] * 3,
        out_specs=pl.BlockSpec(memory_space=pltpu.HBM),
        scratch_shapes=[
            pltpu.VMEM((2, 2 * KEPT, 2 * COLS), BF16),
            pltpu.VMEM((SYSTEMS - TURNED, DEPTH, COLS), BF16),
            pltpu.SemaphoreType.DMA((SYSTEMS,)),
        ],
        compiler_params=pltpu.CompilerParams(vmem_limit_bytes=16 * 2**20),
        name="rotate",
    )(wq, turned, coeffs)


def on_device(basis, image, selection):
    total_rows = basis.shape[1] * lax.axis_size("rows") * lax.axis_size("groups")
    return rotated(*gathered(basis, image, selection, total_rows))


def solution(mesh):
    in_specs = (P(None, ("rows", "groups"), None), P(None, ("rows", "groups"), None), P())
    out_specs = P(None, ("rows", "groups"), None)
    return jax.shard_map(
        on_device, mesh=mesh, in_specs=in_specs, out_specs=out_specs, check_vma=False
    )
```

```python
import functools

import jax
import jax.numpy as jnp
from jax import lax
from jax.experimental import pallas as pl
from jax.experimental.pallas import tpu as pltpu
from jax.sharding import PartitionSpec as P

ITERS = 3
TURNED = 4
F32 = jnp.float32
BF16 = jnp.bfloat16
SYSTEMS = 8
DEPTH = 4096
COLS = 128
KEPT = 64
PLANE = 16


def split(a):
    high = a.astype(BF16)
    rest = a - high.astype(F32)
    middle = rest.astype(BF16)
    return high, middle, (rest - middle.astype(F32)).astype(BF16)


def right_parts(b, over_b):
    b1, b2, b3 = split(b)
    return [jnp.concatenate(pair, axis=over_b) for pair in ((b1, b1), (b2, b2), (b3, b1))]


def dot(a, b, over_a, over_b, parts=None):
    dims = (((over_a,), (over_b,)), ((), ()))
    a1, a2, a3 = split(a)
    a12, a13 = (jnp.concatenate([a1, other], axis=over_a) for other in (a2, a3))
    terms = [
        lax.dot_general(left, right, dims, preferred_element_type=F32)
        for left, right in zip((a12, a12, a13), parts or right_parts(b, over_b))
    ]
    return terms[0] + (terms[1] + terms[2])


def lane(tile, j):
    return jnp.broadcast_to(tile[:, j : j + 1], (8, 128))


def row(tile, j):
    return jnp.broadcast_to(tile[j : j + 1, :], (8, 128))


def added(parts):
    while len(parts) > 1:
        parts = [parts[i] + parts[i + 1] for i in range(0, len(parts), 2)]
    return parts[0]


def times(cols, tile):
    return added([cols[j] * row(tile, j) for j in range(8)])


def less(tile, cols, rows):
    return tile - added([cols[j] * rows[j] for j in range(8)])


def pivot_pair(v, j, sub):
    at, at_next = sub == j, sub == j + 1
    a, b1, b2, c = row(v[j], j), row(v[j + 1], j), row(v[j], j + 1), row(v[j + 1], j + 1)
    r = 1.0 / (a * c - b1 * b2)
    p = jnp.where(at, -1.0, jnp.where(at_next, 0.0, v[j]))
    q = jnp.where(at_next, -1.0, jnp.where(at, 0.0, v[j + 1]))
    v[j], v[j + 1] = r * (q * b2 - p * c), r * (p * b1 - q * a)
    for other in range(8):
        if other not in (j, j + 1):
            u, t = row(v[other], j), row(v[other], j + 1)
            moved = p * (c * u - b1 * t) + q * (a * t - b2 * u)
            v[other] = jnp.where(at | at_next, 0.0, v[other]) - r * moved
    return a, b1, b2, c, r


def stacked(parts):
    return jnp.concatenate(parts, axis=0)


def tiles(a):
    return [a[8 * i : 8 * i + 8] for i in range(a.shape[0] // 8)]


def gauss_jordan(f, x, start, sub):
    for k in range(8):
        v = [lane(f[k], start + 8 * k + j) + 0.0 for j in range(8)]
        cols = {
            i: [lane(f[i], start + 8 * k + j) for j in range(8)]
            for i in [*range(k + 1, 8), *range(k)]
        }
        for j in range(0, 8, 2):
            pivot_pair(v, j, sub)
        fk, xk = times(v, f[k]), times(v, x[k])
        fr = [row(fk, j) for j in range(8)]
        xr = [row(xk, j) for j in range(8)]
        for i in cols:
            f[i] = less(f[i], cols[i], fr)
            x[i] = less(x[i], cols[i], xr)
        f[k], x[k] = fk, xk


def solved(f, x, sub):
    half = f.shape[0] // 2
    left = lax.broadcasted_iota(jnp.int32, (half, 128), 1) < half
    zero = jnp.zeros((half, 128), F32)
    low = f[half:]
    ft, xt = tiles(f[:half]), tiles(x[:half])
    gauss_jordan(ft, xt, 0, sub)
    ft, xt = stacked(ft), stacked(xt)
    right = jnp.concatenate([stacked([ft, zero]), stacked([xt, zero])], axis=1)
    step = dot(jnp.where(left, low, 0.0), right, 1, 0)
    fl, xl = tiles(low - step[:, :128]), tiles(x[half:] - step[:, 128:])
    gauss_jordan(fl, xl, half, sub)
    xl = stacked(xl)
    return stacked([xt - dot(jnp.where(left, 0.0, ft), stacked([zero, xl]), 1, 0), xl])


def next_block(inverse, raw, below):
    g = [added([below[m] * row(inverse[j], m) for m in range(8)]) for j in range(8)]
    return [raw[i] - added([g[j] * row(below[j], i) for j in range(8)]) for i in range(8)]


def normalised_rows(m, y, sub):
    n = len(m)
    out = []
    v = [lane(m[0], j) + 0.0 for j in range(8)]
    for k in range(n):
        if k < n - 1:
            raw = [lane(m[k + 1], 8 * k + 8 + j) + 0.0 for j in range(8)]
        cols = {i: [lane(m[i], 8 * k + j) for j in range(8)] for i in range(k + 1, n)}
        if k < n - 1:
            cols[k + 1] = [c + 0.0 for c in cols[k + 1]]
        mine = y[k]
        scale = jnp.zeros((8, 128), F32)
        for j in range(0, 8, 2):
            p, q = v[j], v[j + 1]
            a, b1, b2, c, r = pivot_pair(v, j, sub)
            inverse_a = 1.0 / a
            g, h = row(mine, j), row(mine, j + 1)
            below = r * (p * (c * g - b1 * h) + q * (a * h - b2 * g))
            mine = mine - jnp.where(
                sub > j + 1, below, jnp.where(sub == j + 1, (b2 * inverse_a) * g, 0.0)
            )
            second = (a * c - b1 * b2) * inverse_a
            scale = jnp.where(sub == j, a, jnp.where(sub == j + 1, second, scale))
        out.append(mine * lax.rsqrt(scale))
        if k < n - 1:
            inverse = v
            v = next_block(inverse, raw, cols[k + 1])
            mk, yk = times(inverse, m[k]), times(inverse, y[k])
            mr = [row(mk, j) for j in range(8)]
            yr = [row(yk, j) for j in range(8)]
            for i in cols:
                m[i] = less(m[i], cols[i], mr)
                y[i] = less(y[i], cols[i], yr)
    return out


def unit_scale(m):
    on = lax.broadcasted_iota(jnp.int32, m.shape, 0) == lax.broadcasted_iota(jnp.int32, m.shape, 1)
    diagonal = jnp.where(on, m, 0.0)
    return [lax.rsqrt(jnp.sum(diagonal, axis=axis, keepdims=True)) for axis in (1, 0)]


HOPS = (2, 0, 1, 3)
ORDER = ((0, 0), (1, 0), (0, 1), (2, 0), (1, 1), (3, 0), (2, 1), (3, 1))
AHEAD = 4
FAR_FIRST = sorted(range(PLANE), key=lambda j: -sum((0, 1, 2, 1)[c] for c in (j // 4, j % 4)))
LANDING = {0: 0, 1: 1, 3: 2}
SENDERS = 3 * PLANE


def system_at(step, x, core):
    k, own = ORDER[step]
    return 2 * lax.rem(x + HOPS[k], 4) + (core if own else 1 - core)


ROTATION_ORDER = tuple(ORDER.index(c) for c in ((1, 1), (1, 0), (2, 1), (2, 0), (3, 1), (3, 0), (0, 1), (0, 0)))


def rotate(both, coeffs, data, out):
    part = 512
    both[:KEPT, :COLS] = coeffs
    both[KEPT:, COLS:] = coeffs
    for at in range(0, DEPTH, part):
        out[at : at + part] = lax.dot_general(
            data[at : at + part], both[...], (((1,), (1,)), ((), ())), preferred_element_type=F32
        ).astype(BF16)


def gather_kernel(
    total_rows, w_hbm, q_hbm, chosen_hbm, out_ref, wq, turned,
    both, chosen_ref, lent, given, sums, relayed, arrived, diagonals, pieces, moves_ref, coeffs, local_coeffs,
    load_sem, lent_sem, given_sem, relay_send, relay_recv, send_sem, recv_sem, diag_send, diag_recv,
    share_send, share_recv, share_diag_send, share_diag_recv, done_send, done_recv, chosen_sem,
):
    me_row, me_group = lax.axis_index("rows"), lax.axis_index("groups")
    x, core = me_group // 2, lax.rem(me_group, 2)
    y, z = me_row // 4, lax.rem(me_row, 4)
    xs, ys, zs = ([lax.rem(c + d, 4) for d in range(4)] for c in (x, y, z))
    row_at = [4 * ys[j // 4] + zs[j % 4] for j in range(PLANE)]
    to_first = 4 * lax.rem(4 - y, 4) + lax.rem(4 - z, 4)

    def device(rows, groups):
        return dict(
            device_id={"rows": rows, "groups": groups}, device_id_type=pl.DeviceIdType.MESH
        )

    def landed(ref, sem):
        pltpu.make_async_copy(ref, ref, sem).wait()

    def load(step):
        s = system_at(step, x, core)
        return [
            pltpu.make_async_copy(ref.at[s], wq.at[step, :, pl.ds(off, COLS)], load_sem.at[step, i])
            for i, (ref, off) in enumerate(((w_hbm, 0), (q_hbm, COLS)))
        ]

    for step in range(AHEAD):
        for copy in load(step):
            copy.start()
    fetch_chosen = pltpu.make_async_copy(chosen_hbm, chosen_ref, chosen_sem)
    fetch_chosen.start()

    barrier = pltpu.get_barrier_semaphore()
    for hop in (1, 3, 2, 0):
        for j in FAR_FIRST if hop != 2 else (0,):
            if hop or j:
                pl.semaphore_signal(barrier, inc=1, **device(row_at[j], 2 * xs[hop] + core))
        pl.semaphore_signal(barrier, inc=1, **device(me_row, 2 * xs[hop] + 1 - core))

    across = lax.broadcasted_iota(jnp.int32, (COLS, COLS), 1)
    down = lax.broadcasted_iota(jnp.int32, (COLS, COLS), 0)

    def gram(step, ref):
        for copy in load(step):
            copy.wait()
        if step + AHEAD < SYSTEMS:
            for copy in load(step + AHEAD):
                copy.start()
        over_rows = (((0,), (0,)), ((), ()))
        w, q = wq[step, :, :COLS], wq[step, :, COLS:]
        gram_s = lax.dot_general(w, w, over_rows, preferred_element_type=F32)
        g = lax.dot_general(q, wq[step], over_rows, preferred_element_type=F32)
        gram_f = g[:, COLS:]
        ref[pl.ds(0, PLANE), 0:8, :] = g[:, :COLS].reshape(PLANE, 8, COLS)
        ref[pl.ds(0, PLANE), 8:16, :] = jnp.where(down >= across, gram_s, gram_f).reshape(
            PLANE, 8, COLS
        )
        diagonal = jnp.sum(jnp.where(down == across, gram_f, 0.0), axis=0, keepdims=True)
        ref[PLANE] = jnp.broadcast_to(diagonal, (16, COLS))

    def lend(k):
        return pltpu.make_async_remote_copy(
            src_ref=lent.at[k], dst_ref=given.at[k], send_sem=lent_sem.at[k],
            recv_sem=given_sem.at[k], **device(me_row, 2 * x + 1 - core),
        )

    def scatter(k):
        hop = HOPS[k]
        target = 2 * xs[hop] + core

        def diagonal():
            pltpu.make_async_remote_copy(
                src_ref=sums.at[k, PLANE, pl.ds(0, 8)], dst_ref=diagonals.at[PLANE * LANDING[hop] + to_first],
                send_sem=diag_send, recv_sem=diag_recv, **device(0, target),
            ).start()

        if hop:
            diagonal()
        else:
            pl.when(me_row != 0)(diagonal)
            arrived[0] = sums[k, me_row]

            @pl.when(me_row == 0)
            def _():
                diagonals[0] = sums[k, PLANE, 0:8]

        for j in FAR_FIRST:
            if hop or j:
                pltpu.make_async_remote_copy(
                    src_ref=sums.at[k, row_at[j]], dst_ref=arrived.at[PLANE * LANDING[hop] + j],
                    send_sem=send_sem, recv_sem=recv_sem, **device(row_at[j], target),
                ).start()

    halves = {3: pl.ds(0, PLANE // 2), 1: pl.ds(PLANE // 2, PLANE // 2 + 1)}

    def relay(hop):
        return pltpu.make_async_remote_copy(
            src_ref=sums.at[0, halves[hop]], dst_ref=relayed.at[halves[hop]],
            send_sem=relay_send.at[hop], recv_sem=relay_recv.at[hop],
            **device(me_row, 2 * xs[hop] + core),
        )

    def combine(k):
        hop = HOPS[k]
        lend(k).wait_recv()
        sums[k] = sums[k] + given[k]
        if hop == 2:
            relay(1).start()
            relay(3).start()
            return
        if hop:
            relay(hop).wait_recv()
            sums[k, halves[hop]] = sums[k, halves[hop]] + relayed[halves[hop]]
        scatter(k)

    for step, (k, own) in enumerate(ORDER):
        gram(step, (sums if own else lent).at[k])
        if step == 0:
            pl.semaphore_wait(barrier, SENDERS - 1 + 5)
        if own:
            combine(k)
        else:
            lend(k).start()

    fetch_chosen.wait()
    chosen = chosen_ref[pl.ds(me_group, 1), :]
    coeffs[...] = (lax.broadcasted_iota(jnp.int32, (COLS, KEPT), 0) == chosen).astype(F32).T

    def share(j, part, send, recv):
        return pltpu.make_async_remote_copy(
            src_ref=part, dst_ref=part, send_sem=send, recv_sem=recv, **device(row_at[j], me_group)
        )

    shared_diagonal = pieces.at[PLANE, pl.ds(0, 8)]

    @pl.when(me_row == 0)
    def _():
        landed(diagonals.at[pl.ds(1, SENDERS - 1)], diag_recv)
        pieces[PLANE, 0:8, :] = lax.fori_loop(
            1, SENDERS, lambda i, total: total + diagonals[i], diagonals[0], unroll=47
        )
        for j in FAR_FIRST[:-1]:
            share(j, shared_diagonal, share_diag_send, share_diag_recv).start()

    others = arrived.at[pl.ds(1, SENDERS - 1)]
    landed(others, recv_sem)

    def add(i, total):
        return total + arrived[i]

    pieces[me_row] = lax.fori_loop(1, SENDERS, add, arrived[0], unroll=47)

    for j in FAR_FIRST[:-1]:
        share(j, pieces.at[me_row], share_send, share_recv).start()
    fifteen = pieces.at[pl.ds(0, PLANE - 1)]

    @pl.when(me_row != 0)
    def _():
        landed(shared_diagonal, share_diag_recv)

    landed(fifteen, share_recv)

    sub = lax.broadcasted_iota(jnp.int32, (8, 128), 0)
    mixed = stacked([pieces[i, 8:16, :] for i in range(PLANE)])
    mixed_t = mixed.T
    diagonal = jnp.broadcast_to(pieces[PLANE, 0:1, :], (COLS, COLS))
    gram_f = jnp.where(down < across, mixed, jnp.where(down == across, diagonal, mixed_t))
    gram_s = jnp.where(down >= across, mixed, mixed_t)
    by_row, by_col = unit_scale(diagonal)
    cross_t = stacked([pieces[i, 0:8, :] for i in range(PLANE)])
    step_matrix = solved(gram_f * by_row * by_col, cross_t * by_row, sub) * by_row
    moves = stacked([step_matrix, dot(gram_s, step_matrix, 1, 0)])

    for i, part in enumerate(right_parts(moves, 1)):
        moves_ref[i] = part

    def iterate(i, _):
        moved = dot(coeffs[...], None, 1, 1, [moves_ref[i] for i in range(3)])
        solution_t, weighted = moved[:, :COLS], moved[:, COLS:]
        metric = dot(solution_t, weighted, 1, 1) * (1.0 / total_rows)
        by_row, by_col = unit_scale(metric)
        metric = metric * by_row * by_col
        wide = jnp.concatenate([metric, jnp.zeros((KEPT, COLS - KEPT), F32)], axis=1)
        coeffs[...] = stacked(normalised_rows(tiles(wide), tiles(solution_t * by_row), sub))
        return 0

    lax.fori_loop(0, ITERS, iterate, 0)
    local_coeffs[...] = coeffs[...].astype(BF16)
    out_ref[me_group] = local_coeffs[...]
    both[...] = jnp.zeros_like(both)

    def tell(hop, same):
        target = 2 * xs[hop] + (core if same else 1 - core)
        return pltpu.make_async_remote_copy(
            src_ref=local_coeffs, dst_ref=out_ref.at[me_group], send_sem=done_send,
            recv_sem=done_recv.at[2 * hop + same], **device(me_row, target),
        )

    for hop, same in ((2, 1), (2, 0), (1, 1), (1, 0), (3, 1), (3, 0), (0, 0)):
        tell(hop, same).start()
    for i, step in enumerate(ROTATION_ORDER):
        k, same = ORDER[step]
        hop = HOPS[k]
        s = system_at(step, x, core)
        if i:
            landed(out_ref.at[s], done_recv.at[2 * ((4 - hop) % 4) + same])
        if i < TURNED:
            rotate(both.at[i % 2], out_ref[s], wq.at[step], turned.at[i])
    landed(out_ref.at[pl.ds(0, SYSTEMS - 1)], done_send)
    landed(fifteen, share_send)
    landed(others, send_sem)
    landed(diagonals.at[pl.ds(0, 2)], diag_send)

    @pl.when(me_row != 0)
    def _():
        landed(shared_diagonal, diag_send)

    @pl.when(me_row == 0)
    def _():
        landed(diagonals.at[pl.ds(0, PLANE - 1)], share_diag_send)

    for k in range(4):
        lend(k).wait_send()
    relay(1).wait_send()
    relay(3).wait_send()


def in_hbm(a):
    return pltpu.with_memory_space_constraint(a, pltpu.HBM)


def gathered(basis, image, selection, total_rows):
    piece = (16, COLS)
    dma = pltpu.SemaphoreType.DMA
    return pl.pallas_call(
        functools.partial(gather_kernel, total_rows),
        out_shape=[
            pltpu.VMEM((SYSTEMS, KEPT, COLS), BF16),
            pltpu.VMEM((SYSTEMS, DEPTH, 2 * COLS), BF16),
            pltpu.VMEM((TURNED, DEPTH, COLS), BF16),
        ],
        in_specs=[pl.BlockSpec(memory_space=pltpu.HBM)] * 3,
        out_specs=[pl.BlockSpec(memory_space=pltpu.VMEM)] * 3,
        scratch_shapes=[
            pltpu.VMEM((2, 2 * KEPT, 2 * COLS), BF16),
            pltpu.VMEM((SYSTEMS, KEPT), jnp.int32),
            pltpu.VMEM((4, PLANE + 1, *piece), F32),
            pltpu.VMEM((4, PLANE + 1, *piece), F32),
            pltpu.VMEM((4, PLANE + 1, *piece), F32),
            pltpu.VMEM((PLANE + 1, *piece), F32),
            pltpu.VMEM((SENDERS, *piece), F32),
            pltpu.VMEM((SENDERS, 8, COLS), F32),
            pltpu.VMEM((PLANE + 1, *piece), F32),
            pltpu.VMEM((3, 2 * COLS, 2 * COLS), BF16),
            pltpu.VMEM((KEPT, COLS), F32),
            pltpu.VMEM((KEPT, COLS), BF16),
            dma((SYSTEMS, 2)),
            dma((4,)),
            dma((4,)),
            dma((4,)),
            dma((4,)),
            *[dma] * 9,
            dma((SYSTEMS,)),
            dma,
        ],
        compiler_params=pltpu.CompilerParams(
            collective_id=0, has_side_effects=True, vmem_limit_bytes=16 * 2**20
        ),
        name="gather_solve",
    )(in_hbm(basis), in_hbm(image), in_hbm(selection))


def rotate_kernel(wq, turned, c_ref, o_hbm, both, out, sem):
    group = lax.axis_index("groups")
    x, core = group // 2, lax.rem(group, 2)

    def store(i):
        source = turned.at[i] if i < TURNED else out.at[i - TURNED]
        return pltpu.make_async_copy(
            source, o_hbm.at[system_at(ROTATION_ORDER[i], x, core)], sem.at[i]
        )

    for i in range(TURNED):
        store(i).start()
    both[...] = jnp.zeros_like(both)
    for i in range(TURNED, SYSTEMS):
        step = ROTATION_ORDER[i]
        coeffs = c_ref[system_at(step, x, core)]
        rotate(both.at[i % 2], coeffs, wq.at[step], out.at[i - TURNED])
        store(i).start()
    for i in range(SYSTEMS):
        store(i).wait()


def rotated(coeffs, wq, turned):
    return pl.pallas_call(
        rotate_kernel,
        out_shape=jax.ShapeDtypeStruct((SYSTEMS, DEPTH, COLS), BF16),
        in_specs=[pl.BlockSpec(memory_space=pltpu.VMEM)] * 3,
        out_specs=pl.BlockSpec(memory_space=pltpu.HBM),
        scratch_shapes=[
            pltpu.VMEM((2, 2 * KEPT, 2 * COLS), BF16),
            pltpu.VMEM((SYSTEMS - TURNED, DEPTH, COLS), BF16),
            pltpu.SemaphoreType.DMA((SYSTEMS,)),
        ],
        compiler_params=pltpu.CompilerParams(vmem_limit_bytes=16 * 2**20),
        name="rotate",
    )(wq, turned, coeffs)


def on_device(basis, image, selection):
    total_rows = basis.shape[1] * lax.axis_size("rows") * lax.axis_size("groups")
    return rotated(*gathered(basis, image, selection, total_rows))


def solution(mesh):
    in_specs = (P(None, ("rows", "groups"), None), P(None, ("rows", "groups"), None), P())
    out_specs = P(None, ("rows", "groups"), None)
    return jax.shard_map(
        on_device, mesh=mesh, in_specs=in_specs, out_specs=out_specs, check_vma=False
    )
```
